256 devices in a mesh: seq: 64 (over y, z, core), tp: 4 (over x).
Axes of the slice: x: 4, y: 4, z: 8, core: 2. Of those that a mesh axis runs over, the one named last changes fastest.
Arguments:
- tokens: bfloat16 [49152, 4096], P('seq'), may hold values from -6 to 6
- query_weight: bfloat16 [4096, 2048], P('seq', 'tp'), may hold values from -0.09375 to 0.09375
- key_weight: bfloat16 [4096, 2048], P('seq', 'tp'), may hold values from -0.09375 to 0.09375
- value_weight: bfloat16 [4096, 2048], P('seq', 'tp'), may hold values from -0.09375 to 0.09375
- gate_weight: bfloat16 [4096, 16], P('seq', 'tp'), may hold values from -0.09375 to 0.09375
- decay_rate: float32 [16], P('tp'), may hold values from 4.0690106e-06 to 0.04
- norm_gain: float32 [2048], P('tp'), may hold values from 0.5 to 1.5
- out_weight: bfloat16 [2048, 4096], P(None, 'tp'), may hold values from -0.125 to 0.125
Outputs:
- mixed: bfloat16 [49152, 4096], P('seq', 'tp')
The draws below stay inside these ranges and needn't reach their ends.
All inputs are finite; a program needn't handle non-finite values.
Results may differ from the reference program's by a relative error of at most 0.006.
The reference program's roundings to bfloat16 on the way count: a program that leaves them out, or rounds other values in their place, can miss the bound.
Values may be sent and summed in bfloat16 or wider, within the bound.
A program may use at most 128 MiB of HBM per device.

```python
import math
import jax
import jax.numpy as jnp
from jax import lax

D = 4096
H = 16
K = 128
TOK_DEV = 768
TOKENS = 49152


def level_of(own_key, shape, shards, smallest, high):
    def one(dim, blocks):
        steps = jax.random.uniform(jax.random.fold_in(jax.random.fold_in(own_key, 6), dim), (blocks,), jnp.float32, smallest / len(shards), high / len(shards))
        return jnp.repeat(jnp.exp(steps), shape[dim] // blocks).reshape((-1,) + (1,) * (len(shape) - dim - 1))

    level = one(*shards[0])
    for cut in shards[1:]:
        level = level * one(*cut)
    return level


def centred(own_key, dims, spread, reach, pieces=(), kind=jnp.bfloat16):
    loudness = level_of(own_key, dims, pieces, -0.22, 0.18) if pieces else 1.0
    values = jax.random.normal(own_key, dims, jnp.float32) * spread * loudness
    return jnp.minimum(jnp.maximum(values, -reach), reach).astype(kind)


def setup_inputs(seed: int = 0) -> dict:
    key_of = jax.random.split(jax.random.key(seed), 9)
    return {
        "tokens": centred(key_of[0], (TOKENS, D), 1.0, 6.0, ((0, 64),)),
        "query_weight": centred(key_of[1], (D, H * K), D ** -0.5, 0.09375, ((0, 64), (1, 4))),
        "key_weight": centred(key_of[2], (D, H * K), D ** -0.5, 0.09375, ((0, 64), (1, 4))),
        "value_weight": centred(key_of[3], (D, H * K), D ** -0.5, 0.09375, ((0, 64), (1, 4))),
        "gate_weight": centred(key_of[4], (D, H), D ** -0.5, 0.09375, ((0, 64), (1, 4))),
        "decay_rate": jnp.clip(jnp.exp(math.log(0.04) - 9.1932348 * jax.random.uniform(key_of[5], (H,), jnp.float32) ** level_of(key_of[5], (H,), ((0, 4),), -0.2, 0.2)), 4.069010628882097e-06, 0.04),
        "norm_gain": jnp.clip(1.0 + 0.1 * jax.random.normal(key_of[6], (H * K,), jnp.float32), 0.5, 1.5),
        "out_weight": centred(key_of[7], (H * K, D), (H * K) ** -0.5, 0.125, ((1, 4),)),
    }


def reference(tokens, query_weight, key_weight, value_weight, gate_weight, decay_rate, norm_gain, out_weight):
    query_proj = jnp.dot(tokens, query_weight, preferred_element_type=jnp.float32).astype(jnp.bfloat16)
    key_proj = jnp.dot(tokens, key_weight, preferred_element_type=jnp.float32).astype(jnp.bfloat16)
    value_proj = jnp.dot(tokens, value_weight, preferred_element_type=jnp.float32).astype(jnp.bfloat16)
    gate_logit = jnp.dot(tokens, gate_weight, preferred_element_type=jnp.float32)
    log_decay = -decay_rate[None, :] * jax.nn.softplus(gate_logit)
    block_count = TOKENS // TOK_DEV
    query_blocks = query_proj.reshape(block_count, TOK_DEV, H, K)
    key_blocks = key_proj.reshape(block_count, TOK_DEV, H, K)
    value_blocks = value_proj.reshape(block_count, TOK_DEV, H, K)
    decay_blocks = log_decay.reshape(block_count, TOK_DEV, H)
    causal = jnp.tril(jnp.ones((TOK_DEV, TOK_DEV), dtype=bool))[None, :, :]

    def block_step(prev_state, items):
        query_blk, key_blk, value_blk, decay_blk = items
        within = jnp.cumsum(decay_blk, axis=0)
        block_total = within[-1]
        query_wide = query_blk.astype(jnp.float32)
        key_wide = key_blk.astype(jnp.float32)
        value_full_width = value_blk.astype(jnp.float32)
        query_scaled = (jnp.exp(within)[:, :, None] * query_wide).astype(jnp.bfloat16)
        state_bfloat = prev_state.astype(jnp.bfloat16)
        carried_state = jnp.einsum('fys,ysu->fyu', query_scaled.astype(jnp.float32), state_bfloat.astype(jnp.float32))
        scores = jnp.einsum('thk,shk->hts', query_wide, key_wide)
        decay_gap = within.T[:, :, None] - within.T[:, None, :]
        attn = jnp.where(causal, scores * jnp.exp(jnp.where(causal, decay_gap, 0.0)), 0.0).astype(jnp.bfloat16)
        local_part = jnp.einsum('hts,shv->thv', attn.astype(jnp.float32), value_full_width)
        key_scaled = (jnp.exp(block_total[None, :] - within)[:, :, None] * key_wide).astype(jnp.bfloat16)
        shard_local_state = jnp.einsum('gfw,gfz->fwz', key_scaled.astype(jnp.float32), value_full_width)
        next_state = jnp.exp(block_total)[:, None, None] * prev_state + shard_local_state
        return (next_state, carried_state + local_part)
    start_state = jnp.zeros((H, K, K), jnp.float32)
    _, head_out = lax.scan(block_step, start_state, (query_blocks, key_blocks, value_blocks, decay_blocks))
    mean_square = lax.optimization_barrier(jnp.mean(head_out * head_out, axis=-1, keepdims=True))
    normed = (head_out * lax.rsqrt(mean_square + 1e-05)).reshape(TOKENS, H * K) * norm_gain[None, :]
    normed = normed.astype(jnp.bfloat16)
    return jnp.dot(normed, out_weight, preferred_element_type=jnp.float32).astype(jnp.bfloat16)
```

```python
import functools

import jax
import jax.numpy as jnp
from jax import lax
from jax.experimental import pallas as pl
from jax.experimental.pallas import tpu as pltpu
from jax.sharding import PartitionSpec as P

NY, NZ = 4, 8
MESH = pl.DeviceIdType.MESH
UNITS = (
    ((1, 0), (2, 0)),
    ((1, 1), (2, 1)),
    ((0, 0), (0, 1)),
    ((1, 2), (2, 2)),
    ((1, 3), (2, 3)),
    ((0, 2), (0, 3)),
)
NU = len(UNITS)
A1, A2, B1, B2 = 0, 4, 12, 20


class Ring:
    def __init__(self, item, n, pos, nxt, prv, recv, send, split=True):
        self.item, self.n, self.pos = item, n, pos
        self.nxt, self.prv, self.recv_sem, self.send_sem = nxt, prv, recv, send
        self.split = split

    def legs(self, r):
        last = r == self.n // 2 - 1
        parts = ((None, None), (0, 1))[last and self.split]
        dirs = (0,) if last and not self.split else (0, 1)
        return [(d, parts[d]) for d in dirs]

    def copy(self, idx, part, r, d):
        ref = self.item(lax.rem(idx + 2 * self.n, self.n), part)
        return pltpu.make_async_remote_copy(
            src_ref=ref,
            dst_ref=ref,
            send_sem=self.send_sem,
            recv_sem=self.recv_sem(2 * r + d),
            device_id=(self.nxt, self.prv)[d],
            device_id_type=MESH,
        )

    def send(self, r):
        for d, part in self.legs(r):
            self.copy(self.pos - r if d == 0 else self.pos + r, part, r, d).start()

    def recv(self, r):
        for d, part in self.legs(r):
            self.copy(
                self.pos - 1 - r if d == 0 else self.pos + 1 + r, part, r, d
            ).wait_recv()


def kernel(
    tok_hbm, wq_hbm, wk_hbm, wv_hbm, gate_hbm,
    proj_ref, logit_ref,
    tok, w, gb, gt, load_sem, recv_sem, send_sem, grecv_sem, gsend_sem, pair_send, pair_recv,
):
    s = lax.axis_index("seq")
    y, z, c = s // (2 * NZ), lax.rem(s // 2, NZ), lax.rem(s, 2)

    def seq_id(yy, zz, cc):
        return {"seq": (lax.rem(yy + NY, NY) * NZ + lax.rem(zz + NZ, NZ)) * 2 + cc}

    yp, ym = seq_id(y + 1, z, c), seq_id(y - 1, z, c)
    zp, zm = seq_id(y, z + 1, c), seq_id(y, z - 1, c)
    mate = seq_id(y, z, 1 - c)

    loads = []
    for u, tiles in enumerate(UNITS):
        for t, (m, h) in enumerate(tiles):
            src = (wq_hbm, wk_hbm, wv_hbm)[m].at[:, h * 128 : (h + 1) * 128]
            loads.append(
                pltpu.make_async_copy(src, w.at[u, t, y, z, c], load_sem.at[u * 2 + t])
            )
    loads.append(pltpu.make_async_copy(gate_hbm, gb.at[y, z, c], load_sem.at[2 * NU]))
    for cp in loads:
        cp.start()
    tok_load = pltpu.make_async_copy(tok_hbm, tok, load_sem.at[2 * NU + 1])
    tok_load.start()

    barrier = pltpu.get_barrier_semaphore()
    for dev in (yp, ym, zp, zm, mate):
        pl.semaphore_signal(barrier, inc=1, device_id=dev, device_id_type=MESH)
    pl.semaphore_wait(barrier, 5)
    for cp in loads:
        cp.wait()

    def rows(part):
        return slice(None) if part is None else pl.ds(part * 32, 32)

    def rings(u):
        def make(base, k, item, along_y):
            return Ring(
                item, NY if along_y else NZ, y if along_y else z,
                yp if along_y else zp, ym if along_y else zm,
                lambda i: recv_sem.at[u, base + i], send_sem.at[u, k],
            )

        return (
            make(A1, 0, lambda i, p: w.at[u, 0, i, z, c, rows(p)], True),
            make(A2, 1, lambda i, p: w.at[u, 0, :, i, c, rows(p)], False),
            make(B1, 2, lambda i, p: w.at[u, 1, y, i, c, rows(p)], False),
            make(B2, 3, lambda i, p: w.at[u, 1, i, :, c, rows(p)], True),
        )

    g1 = Ring(lambda i, p: gb.at[i, z, c], NY, y, yp, ym,
              lambda i: grecv_sem.at[i], gsend_sem.at[0], split=False)
    g2 = Ring(lambda i, p: gb.at[:, i, c], NZ, z, zp, zm,
              lambda i: grecv_sem.at[4 + i], gsend_sem.at[1], split=False)

    def to_mate(ring, idx, k):
        ref = ring.item(lax.rem(idx + 2 * ring.n, ring.n), None)
        pltpu.make_async_remote_copy(
            src_ref=ref, dst_ref=ref, send_sem=pair_send.at[k], recv_sem=pair_recv.at[k],
            device_id=mate, device_id_type=MESH,
        ).start()

    def step(j, u):
        a1, a2, b1, b2 = rings(u)
        first = u == 0
        if j == 0:
            @pl.when(first)
            def _():
                g1.send(0)
            a1.send(0)
            b1.send(0)
        elif j == 1:
            @pl.when(first)
            def _():
                g1.recv(0)
                g1.send(1)
            a1.recv(0)
            a1.send(1)
            b1.recv(0)
            b1.send(1)
        elif j == 2:
            @pl.when(first)
            def _():
                g1.recv(1)
                g2.send(0)
                to_mate(g2, z, NU)
            a1.recv(1)
            a2.send(0)
            to_mate(a2, z, u)
            b1.recv(1)
            b1.send(2)
        elif j == 3:
            @pl.when(first)
            def _():
                g2.recv(0)
                g2.send(1)
                to_mate(g2, z + 1, NU)
                to_mate(g2, z - 1, NU)
            b1.recv(2)
            b1.send(3)
            a2.recv(0)
            a2.send(1)
            to_mate(a2, z + 1, u)
            to_mate(a2, z - 1, u)
        elif j == 4:
            @pl.when(first)
            def _():
                g2.recv(1)
                g2.send(2)
                to_mate(g2, z + 2, NU)
                to_mate(g2, z - 2, NU)
            b1.recv(3)
            b2.send(0)
            to_mate(b2, y, u)
            a2.recv(1)
            a2.send(2)
            to_mate(a2, z + 2, u)
            to_mate(a2, z - 2, u)
        elif j == 5:
            @pl.when(first)
            def _():
                g2.recv(2)
                g2.send(3)
                to_mate(g2, z + 3, NU)
                to_mate(g2, z - 3, NU)
            a2.recv(2)
            a2.send(3)
            to_mate(a2, z + 3, u)
            to_mate(a2, z - 3, u)
            b2.recv(0)
            b2.send(1)
            to_mate(b2, y + 1, u)
            to_mate(b2, y - 1, u)
        elif j == 6:
            @pl.when(first)
            def _():
                g2.recv(3)
                to_mate(g2, z + 4, NU)
            a2.recv(3)
            to_mate(a2, z + 4, u)
            b2.recv(1)
            to_mate(b2, y + 2, u)
        else:
            def pair_done(ref, k):
                return pltpu.make_async_remote_copy(
                    src_ref=ref, dst_ref=ref, send_sem=pair_send.at[k],
                    recv_sem=pair_recv.at[k], device_id=mate, device_id_type=MESH,
                )

            def sent(ref, sem):
                pltpu.make_async_remote_copy(
                    src_ref=ref, dst_ref=ref, send_sem=sem, recv_sem=pair_recv.at[0],
                    device_id=mate, device_id_type=MESH,
                ).wait_send()

            @pl.when(first)
            def _():
                pair_done(gb.at[:, :, 1 - c], NU).wait_recv()
                pair_done(gb.at[:, :, c], NU).wait_send()
                sent(gb.at[pl.ds(0, 3), z, c], gsend_sem.at[0])
                sent(gb.at[:, pl.ds(0, 7), c], gsend_sem.at[1])
            pair_done(w.at[u, :, :, :, 1 - c], u).wait_recv()
            pair_done(w.at[u, :, :, :, c], u).wait_send()
            sent(w.at[u, 0, pl.ds(0, 3), z, c], send_sem.at[u, 0])
            sent(w.at[u, 0, :, pl.ds(0, 7), c], send_sem.at[u, 1])
            sent(w.at[u, 1, y, pl.ds(0, 7), c], send_sem.at[u, 2])
            sent(w.at[u, 1, pl.ds(0, 3), :, c], send_sem.at[u, 3])

    def guarded(j, u):
        @pl.when(jnp.logical_and(u >= 0, u < NU))
        def _():
            step(j, u)

    def project(u):
        rhs = jnp.concatenate(
            [w[u, 0].reshape(4096, 128), w[u, 1].reshape(4096, 128)], axis=1
        )

        def chunk(r, _):
            at = pl.ds(pl.multiple_of(r * 256, 256), 256)
            proj_ref[u, at, :] = jnp.dot(
                tok[at, :], rhs, preferred_element_type=jnp.float32
            ).astype(jnp.bfloat16)
            return 0

        lax.fori_loop(0, 3, chunk, 0)

    def gate():
        gt[...] = jnp.zeros_like(gt)
        for yy in range(NY):
            for zz in range(NZ):
                k = (yy * NZ + zz) * 128
                gt[0:16, k : k + 128] = gb[yy, zz, 0] + gb[yy, zz, 1]
        logit_ref[...] = lax.dot_general(
            tok[...], gt[...], (((1,), (1,)), ((), ())), preferred_element_type=jnp.float32
        )

    def slot(i, _):
        for k in range(4):
            guarded(6 - 2 * k, i - 3 + k)
        for k in range(4):
            guarded(7 - 2 * k, i - 3 + k)

        @pl.when(i == 3)
        def _():
            tok_load.wait()
            gate()

        @pl.when(i >= 3)
        def _():
            project(i - 3)

        return 0

    lax.fori_loop(0, NU + 3, slot, 0)


def fused(tokens, wq, wk, wv, gate):
    rows, depth = tokens.shape
    any_spec = pl.BlockSpec(memory_space=pl.ANY)
    vmem = pl.BlockSpec(memory_space=pltpu.VMEM)
    return pl.pallas_call(
        kernel,
        out_shape=(
            jax.ShapeDtypeStruct((NU, rows, 256), jnp.bfloat16),
            jax.ShapeDtypeStruct((rows, 128), jnp.float32),
        ),
        in_specs=[any_spec] * 5,
        out_specs=(vmem, vmem),
        scratch_shapes=[
            pltpu.VMEM((rows, depth), jnp.bfloat16),
            pltpu.VMEM((NU, 2, NY, NZ, 2, 64, 128), jnp.bfloat16),
            pltpu.VMEM((NY, NZ, 2, 16, 128), jnp.bfloat16),
            pltpu.VMEM((128, depth), jnp.bfloat16),
            pltpu.SemaphoreType.DMA((2 * NU + 2,)),
            pltpu.SemaphoreType.DMA((NU, 24)),
            pltpu.SemaphoreType.DMA((NU, 4)),
            pltpu.SemaphoreType.DMA((12,)),
            pltpu.SemaphoreType.DMA((2,)),
            pltpu.SemaphoreType.DMA((NU + 1,)),
            pltpu.SemaphoreType.DMA((NU + 1,)),
        ],
        compiler_params=pltpu.CompilerParams(
            collective_id=0, has_side_effects=True, vmem_limit_bytes=60 * 1024 * 1024
        ),
    )(tokens, wq, wk, wv, gate)


def decayed_join(earlier, later):
    return (earlier[0] + later[0], jnp.exp(later[0])[:, None, None] * earlier[1] + later[1])


def carried_in(total, state):
    s = lax.axis_index("seq")
    totals = lax.all_gather(total, "seq")
    states = lax.all_gather(state, "seq")
    acc = jnp.zeros_like(state)
    for k in range(64):
        acc = jnp.where(k < s, jnp.exp(totals[k])[:, None, None] * acc + states[k], acc)
    return acc


def on_device(tokens, wq, wk, wv, wg, decay_rate, norm_gain, out_weight):
    rows = tokens.shape[0]
    heads, k = 4, 128
    core = lax.rem(lax.axis_index("seq"), 2)
    gt = wg.T
    blank = jnp.zeros_like(gt)
    gate = jnp.concatenate(
        [jnp.where(core == 0, gt, blank), jnp.where(core == 1, gt, blank)], axis=1
    )
    gate = jnp.pad(gate, ((0, 12), (0, 0)))
    proj, logits = fused(tokens, wq, wk, wv, gate)
    slots = {t: (u, i) for u, tiles in enumerate(UNITS) for i, t in enumerate(tiles)}

    def matrix(m):
        parts = [slots[(m, h)] for h in range(heads)]
        return jnp.stack([proj[u, :, i * 128 : (i + 1) * 128] for u, i in parts], axis=1)

    q, kk, v = matrix(0), matrix(1), matrix(2)
    log_decay = -decay_rate[None, :] * jax.nn.softplus(logits[:, :heads])
    within = jnp.cumsum(log_decay, axis=0)
    total = within[-1]
    ks = (jnp.exp(total[None, :] - within)[:, :, None] * kk).astype(jnp.bfloat16)
    local_state = jnp.einsum("gfw,gfz->fwz", ks, v, preferred_element_type=jnp.float32)
    prefix = carried_in(total, local_state)
    qs = (jnp.exp(within)[:, :, None] * q).astype(jnp.bfloat16)
    carried = jnp.einsum(
        "fys,ysu->fyu", qs, prefix.astype(jnp.bfloat16), preferred_element_type=jnp.float32
    )
    scores = jnp.einsum("thk,shk->hts", q, kk, preferred_element_type=jnp.float32)
    causal = jnp.tril(jnp.ones((rows, rows), dtype=bool))[None]
    gap = within.T[:, :, None] - within.T[:, None, :]
    attn = jnp.where(causal, scores * jnp.exp(jnp.where(causal, gap, 0.0)), 0.0).astype(
        jnp.bfloat16
    )
    local = jnp.einsum("hts,shv->thv", attn, v, preferred_element_type=jnp.float32)
    head_out = carried + local
    ms = jnp.mean(head_out * head_out, axis=-1, keepdims=True)
    normed = (head_out * lax.rsqrt(ms + 1e-05)).reshape(rows, heads * k) * norm_gain[None, :]
    normed = normed.astype(jnp.bfloat16)
    mixed = jnp.dot(
        lax.all_gather(normed, "tp", axis=1, tiled=True), out_weight,
        preferred_element_type=jnp.float32,
    )
    return mixed.astype(jnp.bfloat16)


def solution(mesh):
    return jax.shard_map(
        on_device,
        mesh=mesh,
        in_specs=(
            P("seq", None), P("seq", "tp"), P("seq", "tp"), P("seq", "tp"), P("seq", "tp"),
            P("tp"), P("tp"), P(None, "tp"),
        ),
        out_specs=P("seq", "tp"),
        check_vma=False,
    )
```

```python
import jax
import jax.numpy as jnp
from jax import lax
from jax.experimental import pallas as pl
from jax.experimental.pallas import tpu as pltpu
from jax.sharding import PartitionSpec as P

NX, NY, NZ = 4, 4, 8
MESH = pl.DeviceIdType.MESH
UNITS = (
    ((1, 0), (2, 0)),
    ((1, 1), (2, 1)),
    ((0, 0), (0, 1)),
    ((1, 2), (2, 2)),
    ((1, 3), (2, 3)),
    ((0, 2), (0, 3)),
)
NU = len(UNITS)
NH = 4
A1, A2, B1, B2 = 0, 4, 12, 20


class Ring:
    def __init__(self, item, n, pos, nxt, prv, recv, send, split=True):
        self.item, self.n, self.pos = item, n, pos
        self.nxt, self.prv, self.recv_sem, self.send_sem = nxt, prv, recv, send
        self.split = split

    def legs(self, r):
        last = r == self.n // 2 - 1
        parts = ((None, None), (0, 1))[last and self.split]
        dirs = (0,) if last and not self.split else (0, 1)
        return [(d, parts[d]) for d in dirs]

    def copy(self, idx, part, r, d):
        ref = self.item(lax.rem(idx + 2 * self.n, self.n), part)
        return pltpu.make_async_remote_copy(
            src_ref=ref,
            dst_ref=ref,
            send_sem=self.send_sem,
            recv_sem=self.recv_sem(2 * r + d),
            device_id=(self.nxt, self.prv)[d],
            device_id_type=MESH,
        )

    def send(self, r):
        for d, part in self.legs(r):
            self.copy(self.pos - r if d == 0 else self.pos + r, part, r, d).start()

    def recv(self, r):
        for d, part in self.legs(r):
            self.copy(
                self.pos - 1 - r if d == 0 else self.pos + 1 + r, part, r, d
            ).wait_recv()


def thirds(v):
    hi = v.astype(jnp.bfloat16).astype(jnp.float32)
    mid = (v - hi).astype(jnp.bfloat16).astype(jnp.float32)
    return hi, mid, v - hi - mid


def kernel(
    tok_hbm, wq_hbm, wk_hbm, wv_hbm, gate_hbm, ow_hbm, rate_ref, gain_ref,
    out_ref,
    tok, w, gb, gt, ow, proj, wcol, wrow, total, loc, swap, tz, ty, hand, state, local,
    qs, nb, acc,
    load_sem, recv_sem, send_sem, grecv_sem, gsend_sem, pair_send, pair_recv,
    swap_sem, zs_sem, zr_sem, ys_sem, yr_sem, hand_sem, xs_sem, xr_sem,
):
    x = lax.axis_index("tp")
    s = lax.axis_index("seq")
    y, z, c = s // (2 * NZ), lax.rem(s // 2, NZ), lax.rem(s, 2)

    def seq_id(yy, zz, cc):
        return {"seq": (lax.rem(yy + NY, NY) * NZ + lax.rem(zz + NZ, NZ)) * 2 + cc}

    yp, ym = seq_id(y + 1, z, c), seq_id(y - 1, z, c)
    zp, zm = seq_id(y, z + 1, c), seq_id(y, z - 1, c)
    mate = seq_id(y, z, 1 - c)
    xp, xm = {"tp": lax.rem(x + 1, NX)}, {"tp": lax.rem(x + NX - 1, NX)}

    loads = []
    for u, tiles in enumerate(UNITS):
        for t, (m, h) in enumerate(tiles):
            src = (wq_hbm, wk_hbm, wv_hbm)[m].at[:, h * 128 : (h + 1) * 128]
            loads.append(
                pltpu.make_async_copy(src, w.at[u, t, y, z, c], load_sem.at[u * 2 + t])
            )
    loads.append(pltpu.make_async_copy(gate_hbm, gb.at[y, z, c], load_sem.at[2 * NU]))
    for cp in loads:
        cp.start()
    tok_load = pltpu.make_async_copy(tok_hbm, tok, load_sem.at[2 * NU + 1])
    tok_load.start()
    ow_load = pltpu.make_async_copy(ow_hbm, ow, load_sem.at[2 * NU + 2])
    ow_load.start()

    barrier = pltpu.get_barrier_semaphore()
    for dev in (yp, ym, zp, zm, mate, xp, xm):
        pl.semaphore_signal(barrier, inc=1, device_id=dev, device_id_type=MESH)
    pl.semaphore_wait(barrier, 7)
    for cp in loads:
        cp.wait()

    def rows(part):
        return slice(None) if part is None else pl.ds(part * 32, 32)

    def rings(u):
        def make(base, k, item, along_y):
            return Ring(
                item, NY if along_y else NZ, y if along_y else z,
                yp if along_y else zp, ym if along_y else zm,
                lambda i: recv_sem.at[u, base + i], send_sem.at[u, k],
            )

        return (
            make(A1, 0, lambda i, p: w.at[u, 0, i, z, c, rows(p)], True),
            make(A2, 1, lambda i, p: w.at[u, 0, :, i, c, rows(p)], False),
            make(B1, 2, lambda i, p: w.at[u, 1, y, i, c, rows(p)], False),
            make(B2, 3, lambda i, p: w.at[u, 1, i, :, c, rows(p)], True),
        )

    g1 = Ring(lambda i, p: gb.at[i, z, c], NY, y, yp, ym,
              lambda i: grecv_sem.at[i], gsend_sem.at[0], split=False)
    g2 = Ring(lambda i, p: gb.at[:, i, c], NZ, z, zp, zm,
              lambda i: grecv_sem.at[4 + i], gsend_sem.at[1], split=False)

    def to_mate(ring, idx, k):
        ref = ring.item(lax.rem(idx + 2 * ring.n, ring.n), None)
        pltpu.make_async_remote_copy(
            src_ref=ref, dst_ref=ref, send_sem=pair_send.at[k], recv_sem=pair_recv.at[k],
            device_id=mate, device_id_type=MESH,
        ).start()

    def hop(ring, r):
        if r > 0:
            ring.recv(r - 1)
        if r < ring.n // 2:
            ring.send(r)

    def each(body):
        def one(u, _):
            body(u, rings(u))
            return 0

        lax.fori_loop(0, NU, one, 0)

    def spread():
        g1.send(0)

        def first(u, ring):
            ring[0].send(0)
            ring[2].send(0)

        each(first)
        hop(g1, 1)

        def second(u, ring):
            hop(ring[0], 1)
            hop(ring[2], 1)

        each(second)
        hop(g1, 2)
        g2.send(0)
        to_mate(g2, z, NU)

        def third(u, ring):
            hop(ring[0], 2)
            hop(ring[2], 2)

        each(third)
        a_step(0, 0)
        hop(g2, 1)
        to_mate(g2, z + 1, NU)
        to_mate(g2, z - 1, NU)
        each(lambda u, ring: hop(ring[2], 3))
        a_step(0, 1)
        hop(g2, 2)
        to_mate(g2, z + 2, NU)
        to_mate(g2, z - 2, NU)

        def fifth(u, ring):
            hop(ring[2], 4)

            @pl.when(u == 0)
            def _():
                b_step(0, 0)

        each(fifth)
        a_step(1, 0)
        hop(g2, 3)
        to_mate(g2, z + 3, NU)
        to_mate(g2, z - 3, NU)

    def a_step(r, u):
        ring = rings(u)[1]
        hop(ring, r)
        if r == 0:
            to_mate(ring, z, u)
        elif r < 4:
            to_mate(ring, z + r, u)
            to_mate(ring, z - r, u)
        else:
            to_mate(ring, z + 4, u)

    def b_step(r, u):
        ring = rings(u)[3]
        hop(ring, r)
        if r == 0:
            to_mate(ring, y, u)
        elif r == 1:
            to_mate(ring, y + 1, u)
            to_mate(ring, y - 1, u)
        else:
            to_mate(ring, y + 2, u)

    def valid(fn, u):
        @pl.when(jnp.logical_and(u >= 0, u < NU))
        def _():
            fn(u)

    def tick(t):
        for r in range(4, -1, -1):
            valid(lambda u, r=r: a_step(r, u), t + 2 - r)
            if r < 3:
                valid(lambda u, r=r: b_step(r, u), t + 1 - r)

    def pair_done(ref, k):
        return pltpu.make_async_remote_copy(
            src_ref=ref, dst_ref=ref, send_sem=pair_send.at[k], recv_sem=pair_recv.at[k],
            device_id=mate, device_id_type=MESH,
        )

    def sent(ref, sem):
        pltpu.make_async_remote_copy(
            src_ref=ref, dst_ref=ref, send_sem=sem, recv_sem=pair_recv.at[0],
            device_id=mate, device_id_type=MESH,
        ).wait_send()

    def gate_end():
        hop(g2, 4)
        to_mate(g2, z + 4, NU)
        pair_done(gb.at[:, :, 1 - c], NU).wait_recv()

    def finish():
        pair_done(gb.at[:, :, c], NU).wait_send()
        sent(gb.at[pl.ds(0, 3), z, c], gsend_sem.at[0])
        sent(gb.at[:, pl.ds(0, 7), c], gsend_sem.at[1])

        def one(u, ring):
            pair_done(w.at[u, :, :, :, c], u).wait_send()
            sent(w.at[u, 0, pl.ds(0, 3), z, c], send_sem.at[u, 0])
            sent(w.at[u, 0, :, pl.ds(0, 7), c], send_sem.at[u, 1])
            sent(w.at[u, 1, y, pl.ds(0, 7), c], send_sem.at[u, 2])
            sent(w.at[u, 1, pl.ds(0, 3), :, c], send_sem.at[u, 3])

        each(one)

    def project(u):
        rhs = jnp.concatenate(
            [w[u, 0].reshape(4096, 128), w[u, 1].reshape(4096, 128)], axis=1
        )

        def chunk(r, _):
            at = pl.ds(pl.multiple_of(r * 256, 256), 256)
            proj[u, at, :] = jnp.dot(
                tok[at, :], rhs, preferred_element_type=jnp.float32
            ).astype(jnp.bfloat16)
            return 0

        lax.fori_loop(0, 3, chunk, 0)

    def gate():
        gt[...] = jnp.zeros_like(gt)
        for yy in range(NY):
            for zz in range(NZ):
                k = (yy * NZ + zz) * 128
                gt[0:16, k : k + 128] = gb[yy, zz, 0] + gb[yy, zz, 1]
        logit = lax.dot_general(
            tok[...], gt[...], (((1,), (1,)), ((), ())), preferred_element_type=jnp.float32
        )
        logit = logit.T[0:8, :]
        soft = jnp.maximum(logit, 0.0) + jnp.log1p(jnp.exp(-jnp.abs(logit)))
        decay = -rate_ref[:, 0:1] * soft
        hi, mid, lo = thirds(decay)
        parts = jnp.concatenate([hi, mid, lo, jnp.zeros_like(lo)], axis=0).astype(jnp.bfloat16)
        before = lax.broadcasted_iota(jnp.int32, (768, 768), 0)
        after = lax.broadcasted_iota(jnp.int32, (768, 768), 1)
        upper = jnp.where(before <= after, 1.0, 0.0).astype(jnp.bfloat16)
        sums = jnp.dot(parts, upper, preferred_element_type=jnp.float32)
        within = sums[0:8] + sums[8:16] + sums[16:24]
        column = jnp.concatenate([within, jnp.zeros((120, 768), jnp.float32)], axis=0).T
        for h in range(NH):
            wrow[h] = jnp.broadcast_to(within[h : h + 1, :], (8, 768))
            wcol[h] = jnp.broadcast_to(column[:, h : h + 1], (768, 128))
            total[h] = jnp.broadcast_to(within[h : h + 1, 767:768], (8, 128))

    def half(k):
        return pl.ds(pl.multiple_of(k * 64, 64), 64)

    def local_state(u, h):
        key = proj[u, :, 0:128].astype(jnp.float32)
        scaled = (jnp.exp(total[h, 0:1, :] - wcol[h]) * key).astype(jnp.bfloat16)
        loc[h] = lax.dot_general(
            scaled, proj[u, :, 128:256], (((0,), (0,)), ((), ())),
            preferred_element_type=jnp.float32,
        )
        swap[h, 0, 0:64, :] = loc[h, half(1 - c), :]
        swap[h, 0, 64:72, :] = total[h]
        swap_copy(h).start()

    def swap_copy(h):
        return pltpu.make_async_remote_copy(
            src_ref=swap.at[h, 0], dst_ref=swap.at[h, 1], send_sem=swap_sem.at[h, 0],
            recv_sem=swap_sem.at[h, 1], device_id=mate, device_id_type=MESH,
        )

    def hand_copy(h, k):
        return pltpu.make_async_remote_copy(
            src_ref=hand.at[h], dst_ref=state.at[h, half(k)], send_sem=hand_sem.at[h, 0],
            recv_sem=hand_sem.at[h, 1], device_id=mate, device_id_type=MESH,
        )

    def z_ring(h):
        return Ring(lambda i, p: tz.at[h, i], NZ, z, zp, zm,
                    lambda i: zr_sem.at[h, i], zs_sem.at[h], split=False)

    def y_ring(h):
        return Ring(lambda i, p: ty.at[h, i], NY, y, yp, ym,
                    lambda i: yr_sem.at[h, i], ys_sem.at[h], split=False)

    def x_ring(h):
        def item(i, p):
            return nb.at[h, i] if p is None else nb.at[h, i, pl.ds(p * 384, 384)]

        return Ring(item, NX, x, xp, xm, lambda i: xr_sem.at[h, i], xs_sem.at[h])

    def pack(ref, i, value, log):
        hi, mid, lo = thirds(log)
        row = lax.broadcasted_iota(jnp.int32, (16, 128), 0)
        tail = jnp.where(row == 0, hi, jnp.where(row == 1, mid, jnp.where(row == 2, lo, 0.0)))
        ref[i, 0:64, :] = value.astype(jnp.bfloat16)
        ref[i, 64:80, :] = tail.astype(jnp.bfloat16)

    def unpack(ref, i):
        tail = ref[i, 64:80, :].astype(jnp.float32)
        return ref[i, 0:64, :].astype(jnp.float32), jnp.sum(tail, axis=0, keepdims=True)

    def pair(h):
        mine, theirs = loc[h, half(c), :], swap[h, 1, 0:64, :]
        own, other = total[h, 0:1, :], swap[h, 1, 64:65, :]
        first = c == 0
        return (
            jnp.where(first, mine, theirs), jnp.where(first, own, other),
            jnp.where(first, theirs, mine), jnp.where(first, other, own),
        )

    def below(ref, n, limit):
        acc_s = jnp.zeros((64, 128), jnp.float32)
        acc_a = jnp.zeros((1, 128), jnp.float32)
        kept = (acc_s, acc_a)
        for i in range(n):
            s_i, a_i = unpack(ref, i)
            acc_s, acc_a = jnp.exp(a_i) * acc_s + s_i, acc_a + a_i
            kept = tuple(
                jnp.where(i < limit, new, old) for new, old in zip((acc_s, acc_a), kept)
            )
        return kept, (acc_s, acc_a)

    def scan_step(k, h):
        zr, yr = z_ring(h), y_ring(h)
        if k == 1:
            swap_copy(h).wait_recv()
            s0, a0, s1, a1 = pair(h)
            pack(tz.at[h], z, jnp.exp(a1) * s0 + s1, a0 + a1)
            zr.send(0)
        elif k <= 4:
            hop(zr, k - 1)
        elif k == 5:
            hop(zr, 4)
            _, (row_s, row_a) = below(tz.at[h], NZ, z)
            pack(ty.at[h], y, row_s, row_a)
            yr.send(0)
        elif k == 6:
            hop(yr, 1)
        elif k == 7:
            hop(yr, 2)
            (in_s, in_a), _ = below(tz.at[h], NZ, z)
            (row_s, _), _ = below(ty.at[h], NY, y)
            p0 = jnp.exp(in_a) * row_s + in_s
            s0, a0, _, _ = pair(h)
            p1 = jnp.exp(a0) * p0 + s0
            first = c == 0
            hand[h] = jnp.where(first, p1, p0).astype(jnp.bfloat16)
            hand_copy(h, c).start()
            state[h, half(c), :] = jnp.where(first, p0, p1).astype(jnp.bfloat16)
        else:
            hand_copy(h, 1 - c).wait_recv()

    def attention(u, i, h):
        kv = u - 2 + i
        for r in range(3):
            lo, n = r * 256, (r + 1) * 256
            query = proj[u, lo:n, i * 128 : (i + 1) * 128]
            scores = lax.dot_general(
                query, proj[kv, 0:n, 0:128], (((1,), (1,)), ((), ())),
                preferred_element_type=jnp.float32,
            )
            col = wcol[h, lo:n, :]
            gap = jnp.concatenate([col] * (n // 128), axis=1) - wrow[h, 0:1, 0:n]
            t_at = lax.broadcasted_iota(jnp.int32, (256, n), 0) + lo
            s_at = lax.broadcasted_iota(jnp.int32, (256, n), 1)
            causal = s_at <= t_at
            attn = jnp.where(
                causal, scores * jnp.exp(jnp.where(causal, gap, 0.0)), 0.0
            ).astype(jnp.bfloat16)
            local[h, lo:n, :] = jnp.dot(
                attn, proj[kv, 0:n, 128:256], preferred_element_type=jnp.float32
            )
            qs[h, lo:n, :] = (jnp.exp(col) * query.astype(jnp.float32)).astype(jnp.bfloat16)

    def normed(h):
        out = local[h] + jnp.dot(qs[h], state[h], preferred_element_type=jnp.float32)
        scale = lax.rsqrt(jnp.mean(out * out, axis=-1, keepdims=True) + 1e-05)
        nb[h, x] = (out * scale * gain_ref[h, 0:1, :]).astype(jnp.bfloat16)
        x_ring(h).send(0)

    def mix(h, first, last):
        weight = ow[:, h].reshape(512, 1024)

        def chunk(r, _):
            at = pl.ds(pl.multiple_of(r * 256, 256), 256)
            lhs = jnp.concatenate([nb[h, i, at, :] for i in range(NX)], axis=1)
            part = jnp.dot(lhs, weight, preferred_element_type=jnp.float32)
            if not first:
                part = part + acc[at, :]
            if last:
                out_ref[at, :] = part.astype(jnp.bfloat16)
            else:
                acc[at, :] = part
            return 0

        lax.fori_loop(0, 3, chunk, 0)

    def head_at(u, fn):
        @pl.when((u >= 0) & (u <= 4) & (u != 2))
        def _():
            fn(u - u // 3)

    def point(t, p):
        for k in range(8, 0, -1):
            if (10 + k - p) % 3 == 0:
                head_at(t - (10 + k - p) // 3, lambda h, k=k: scan_step(k, h))

    spread()

    def slot(t, _):
        point(t, 0)
        head_at(t - 6, normed)
        head_at(t - 7, lambda h: hop(x_ring(h), 1))

        @pl.when(t < NU + 3)
        def _():
            tick(t)

        point(t, 1)

        @pl.when(t == 1)
        def _():
            gate_end()
            tok_load.wait()
            gate()

        u = t - 3

        @pl.when((u >= 0) & (u < NU))
        def _():
            pair_done(w.at[u, :, :, :, 1 - c], u).wait_recv()
            project(u)
            head_at(u, lambda h: local_state(u, h))

            @pl.when(lax.rem(u, 3) == 2)
            def _():
                for i in range(2):
                    attention(u, i, (u // 3) * 2 + i)

        point(t, 2)

        def gathered(h):
            hop(x_ring(h), 2)

            @pl.when(h == 0)
            def _():
                ow_load.wait()
                mix(h, True, False)

            @pl.when((h > 0) & (h < NH - 1))
            def _():
                mix(h, False, False)

            @pl.when(h == NH - 1)
            def _():
                mix(h, False, True)

        head_at(t - 8, gathered)
        return 0

    lax.fori_loop(0, 13, slot, 0)
    finish()

    def end(h, _):
        swap_copy(h).wait_send()
        sent(tz.at[h, pl.ds(0, 7)], zs_sem.at[h])
        sent(ty.at[h, pl.ds(0, 3)], ys_sem.at[h])
        hand_copy(h, c).wait_send()
        sent(nb.at[h, pl.ds(0, 3)], xs_sem.at[h])
        return 0

    lax.fori_loop(0, NH, end, 0)


def fused(tokens, wq, wk, wv, gate, ow, rate, gain):
    rows, depth = tokens.shape
    any_spec = pl.BlockSpec(memory_space=pl.ANY)
    vmem = pl.BlockSpec(memory_space=pltpu.VMEM)
    bf16, f32, dma = jnp.bfloat16, jnp.float32, pltpu.SemaphoreType.DMA
    return pl.pallas_call(
        kernel,
        out_shape=jax.ShapeDtypeStruct((rows, ow.shape[-1]), bf16),
        in_specs=[any_spec] * 6 + [vmem] * 2,
        out_specs=vmem,
        scratch_shapes=[
            pltpu.VMEM((rows, depth), bf16),
            pltpu.VMEM((NU, 2, NY, NZ, 2, 64, 128), bf16),
            pltpu.VMEM((NY, NZ, 2, 16, 128), bf16),
            pltpu.VMEM((128, depth), bf16),
            pltpu.VMEM(ow.shape, bf16),
            pltpu.VMEM((NU, rows, 256), bf16),
            pltpu.VMEM((NH, rows, 128), f32),
            pltpu.VMEM((NH, 8, rows), f32),
            pltpu.VMEM((NH, 8, 128), f32),
            pltpu.VMEM((NH, 128, 128), f32),
            pltpu.VMEM((NH, 2, 72, 128), f32),
            pltpu.VMEM((NH, NZ, 80, 128), bf16),
            pltpu.VMEM((NH, NY, 80, 128), bf16),
            pltpu.VMEM((NH, 64, 128), bf16),
            pltpu.VMEM((NH, 128, 128), bf16),
            pltpu.VMEM((NH, rows, 128), f32),
            pltpu.VMEM((NH, rows, 128), bf16),
            pltpu.VMEM((NH, NX, rows, 128), bf16),
            pltpu.VMEM((rows, ow.shape[-1]), f32),
            dma((2 * NU + 3,)), dma((NU, 24)), dma((NU, 4)), dma((12,)), dma((2,)),
            dma((NU + 1,)), dma((NU + 1,)),
            dma((NH, 2)), dma((NH,)), dma((NH, 8)), dma((NH,)), dma((NH, 4)), dma((NH, 2)),
            dma((NH,)), dma((NH, 4)),
        ],
        compiler_params=pltpu.CompilerParams(
            collective_id=0, has_side_effects=True, vmem_limit_bytes=63 * 1024 * 1024
        ),
    )(tokens, wq, wk, wv, gate, ow, rate, gain)


def on_device(tokens, wq, wk, wv, wg, decay_rate, norm_gain, out_weight):
    core = lax.rem(lax.axis_index("seq"), 2)
    gt = wg.T
    blank = jnp.zeros_like(gt)
    gate = jnp.concatenate(
        [jnp.where(core == 0, gt, blank), jnp.where(core == 1, gt, blank)], axis=1
    )
    gate = jnp.pad(gate, ((0, 12), (0, 0)))
    rate = jnp.broadcast_to(jnp.pad(decay_rate, (0, 4))[:, None], (8, 128))
    gain = jnp.broadcast_to(norm_gain.reshape(NH, 1, 128), (NH, 8, 128))
    ow = out_weight.reshape(NX, NH, 128, out_weight.shape[1])
    return fused(tokens, wq, wk, wv, gate, ow, rate, gain)


def solution(mesh):
    return jax.shard_map(
        on_device,
        mesh=mesh,
        in_specs=(
            P("seq", None), P("seq", "tp"), P("seq", "tp"), P("seq", "tp"), P("seq", "tp"),
            P("tp"), P("tp"), P(None, "tp"),
        ),
        out_specs=P("seq", "tp"),
        check_vma=False,
    )
```

```python
import jax
import jax.numpy as jnp
from jax import lax
from jax.experimental import pallas as pl
from jax.experimental.pallas import tpu as pltpu
from jax.sharding import PartitionSpec as P

NX, NY, NZ = 4, 4, 8
MESH = pl.DeviceIdType.MESH
UNITS = (
    ((1, 0), (2, 0)),
    ((1, 1), (2, 1)),
    ((1, 2), (2, 2)),
    ((1, 3), (2, 3)),
    ((0, 0), (0, 1)),
    ((0, 2), (0, 3)),
)
NU = len(UNITS)
NH = 4
NB = NU // 2
A1, A2, B1, B2 = 0, 4, 12, 20


class Ring:
    def __init__(self, item, n, pos, nxt, prv, recv, send, split=True):
        self.item, self.n, self.pos = item, n, pos
        self.nxt, self.prv, self.recv_sem, self.send_sem = nxt, prv, recv, send
        self.split = split

    def legs(self, r):
        last = r == self.n // 2 - 1
        parts = ((None, None), (0, 1))[last and self.split]
        dirs = (0,) if last and not self.split else (0, 1)
        return [(d, parts[d]) for d in dirs]

    def copy(self, idx, part, r, d):
        ref = self.item(lax.rem(idx + 2 * self.n, self.n), part)
        return pltpu.make_async_remote_copy(
            src_ref=ref,
            dst_ref=ref,
            send_sem=self.send_sem,
            recv_sem=self.recv_sem(2 * r + d),
            device_id=(self.nxt, self.prv)[d],
            device_id_type=MESH,
        )

    def send(self, r):
        for d, part in self.legs(r):
            self.copy(self.pos - r if d == 0 else self.pos + r, part, r, d).start()

    def recv(self, r):
        for d, part in self.legs(r):
            self.copy(
                self.pos - 1 - r if d == 0 else self.pos + 1 + r, part, r, d
            ).wait_recv()


def thirds(v):
    hi = v.astype(jnp.bfloat16).astype(jnp.float32)
    mid = (v - hi).astype(jnp.bfloat16).astype(jnp.float32)
    return hi, mid, v - hi - mid


def kernel(
    tok_hbm, wq_hbm, wk_hbm, wv_hbm, ow_hbm, gate_ref, rate_ref, gain_ref,
    out_ref,
    tok, w, gb, gt, ow, proj, wcol, wrow, total, loc, swap, tz, ty, hand, state, local,
    qs, nb, acc,
    load_sem, recv_sem, send_sem, grecv_sem, gsend_sem, pair_send, pair_recv,
    swap_sem, zs_sem, zr_sem, ys_sem, yr_sem, hand_sem, xs_sem, xr_sem,
):
    x = lax.axis_index("tp")
    s = lax.axis_index("seq")
    y, z, c = s // (2 * NZ), lax.rem(s // 2, NZ), lax.rem(s, 2)

    def seq_id(yy, zz, cc):
        return {"seq": (lax.rem(yy + NY, NY) * NZ + lax.rem(zz + NZ, NZ)) * 2 + cc}

    yp, ym = seq_id(y + 1, z, c), seq_id(y - 1, z, c)
    zp, zm = seq_id(y, z + 1, c), seq_id(y, z - 1, c)
    mate = seq_id(y, z, 1 - c)
    xp, xm = {"tp": lax.rem(x + 1, NX)}, {"tp": lax.rem(x + NX - 1, NX)}

    loads = []
    for u, tiles in enumerate(UNITS):
        for t, (m, h) in enumerate(tiles):
            src = (wq_hbm, wk_hbm, wv_hbm)[m].at[:, h * 128 : (h + 1) * 128]
            loads.append(
                pltpu.make_async_copy(src, w.at[u, t, y, z, c], load_sem.at[u * 2 + t])
            )
    for cp in loads:
        cp.start()
    tok_load = pltpu.make_async_copy(tok_hbm, tok, load_sem.at[2 * NU + 1])
    tok_load.start()
    ow_load = pltpu.make_async_copy(ow_hbm, ow, load_sem.at[2 * NU + 2])
    ow_load.start()

    barrier = pltpu.get_barrier_semaphore()
    partners = [seq_id(y, z + d, c) for d in range(1, NZ)]
    partners += [seq_id(y + d, z, c) for d in range(1, NY)]
    partners += [mate, xp, xm]
    for dev in partners:
        pl.semaphore_signal(barrier, inc=1, device_id=dev, device_id_type=MESH)
    pl.semaphore_wait(barrier, len(partners))

    def rows(part):
        return slice(None) if part is None else pl.ds(part * 32, 32)

    def piece(b, tile, yy, zz, part):
        return w.at[pl.ds(2 * b, 2), tile, lax.rem(yy + NY, NY), lax.rem(zz + NZ, NZ), c, rows(part)]

    def rings(b):
        made = []

        def make(item, along_y, wait):
            count = len(made)
            base = (0, 4, 12, 20, 28, 36)[count] if count < 6 else 44 + 4 * (count - 6)
            made.append((wait, Ring(
                item, NY if along_y else NZ, y if along_y else z,
                yp if along_y else zp, ym if along_y else zm,
                lambda i: recv_sem.at[b, base + i], send_sem.at[b, count if count < 2 else 2 if count < 6 else 3],
            )))

        make(lambda i, p: piece(b, 0, i, z, p), True, 0)
        make(lambda i, p: piece(b, 1, y, i, p), False, 0)
        for d in (0, 1, -1, 2):
            make(lambda i, p, d=d: piece(b, 0, y + d, i, p), False, abs(d))
        for d in (0, 1, -1, 2, -2, 3, -3, 4):
            make(lambda i, p, d=d: piece(b, 1, i, z + d, p), True, abs(d))
        return made

    g1 = Ring(lambda i, p: gb.at[i, z, c], NY, y, yp, ym,
              lambda i: grecv_sem.at[i], gsend_sem.at[0], split=False)
    g2 = Ring(lambda i, p: gb.at[:, i, c], NZ, z, zp, zm,
              lambda i: grecv_sem.at[4 + i], gsend_sem.at[1], split=False)

    def to_mate(ring, idx, k):
        ref = ring.item(lax.rem(idx + 2 * ring.n, ring.n), None)
        pltpu.make_async_remote_copy(
            src_ref=ref, dst_ref=ref, send_sem=pair_send.at[k], recv_sem=pair_recv.at[k],
            device_id=mate, device_id_type=MESH,
        ).start()

    def hop(ring, r):
        if r > 0:
            ring.recv(r - 1)
        if r < ring.n // 2:
            ring.send(r)

    def load_gate():
        k = lax.broadcasted_iota(jnp.int32, (64, 128), 0)
        lane = lax.broadcasted_iota(jnp.int32, (64, 128), 1)
        pick = jnp.where(lane == k + 64 * c, 1.0, 0.0).astype(jnp.bfloat16)
        turned = lax.dot_general(
            gate_ref[...], pick, (((0,), (0,)), ((), ())), preferred_element_type=jnp.float32
        )
        gb[y, z, c] = jnp.concatenate(
            [turned, jnp.zeros((12, 128), jnp.float32)], axis=0
        ).astype(jnp.bfloat16)

    def column(b, zz):
        ref = w.at[pl.ds(2 * b, 2), :, :, lax.rem(zz + NZ, NZ), c]
        pltpu.make_async_remote_copy(
            src_ref=ref, dst_ref=ref, send_sem=pair_send.at[b], recv_sem=pair_recv.at[b],
            device_id=mate, device_id_type=MESH,
        ).start()

    def gate_round(k):
        if k <= 2:
            hop(g1, k)
        if k >= 2:
            hop(g2, k - 2)
            d = k - 2
            for at in {0: (z,), 4: (z + 4,)}.get(d, (z + d, z - d)):
                to_mate(g2, at, NB)

    def weight_round(k, b):
        if k == 0:
            for i in range(2):
                for t in range(2):
                    own = w.at[2 * b + i, t, y, z, c]
                    pltpu.make_async_copy(own, own, load_sem.at[b * 4 + 2 * i + t]).wait()

            @pl.when(b == 0)
            def _():
                load_gate()

        @pl.when(b == 0)
        def _():
            gate_round(k)

        todo = [(ring, k - wait) for wait, ring in rings(b)]
        for ring, r in todo:
            if 0 < r <= ring.n // 2:
                ring.recv(r - 1)
            if 0 <= r < ring.n // 2:
                ring.send(r)
        if k >= 2:
            d = k - 2
            for at in {0: (z,), 4: (z + 4,)}.get(d, (z + d, z - d)):
                column(b, at)

    def valid(k, b):
        @pl.when((b >= 0) & (b < NB))
        def _():
            weight_round(k, b)

    def pair_done(ref, k):
        return pltpu.make_async_remote_copy(
            src_ref=ref, dst_ref=ref, send_sem=pair_send.at[k], recv_sem=pair_recv.at[k],
            device_id=mate, device_id_type=MESH,
        )

    def sent(ref, sem):
        pltpu.make_async_remote_copy(
            src_ref=ref, dst_ref=ref, send_sem=sem, recv_sem=pair_recv.at[0],
            device_id=mate, device_id_type=MESH,
        ).wait_send()

    def finish():
        pair_done(gb.at[:, :, c], NB).wait_send()
        sent(gb.at[pl.ds(0, 3), z, c], gsend_sem.at[0])
        sent(gb.at[:, pl.ds(0, 7), c], gsend_sem.at[1])

        def one(b, _):
            two = pl.ds(2 * b, 2)
            pair_done(w.at[two, :, :, :, c], b).wait_send()
            sent(w.at[two, 0, pl.ds(0, 3), z, c], send_sem.at[b, 0])
            sent(w.at[two, 1, y, pl.ds(0, 7), c], send_sem.at[b, 1])
            sent(w.at[two, 0, :, pl.ds(0, 7), c], send_sem.at[b, 2])
            sent(w.at[two, 1, pl.ds(0, 3), :, c], send_sem.at[b, 3])
            return 0

        lax.fori_loop(0, NB, one, 0)

    def project(u):
        rhs = jnp.concatenate(
            [w[u, 0].reshape(4096, 128), w[u, 1].reshape(4096, 128)], axis=1
        )

        def chunk(r, _):
            at = pl.ds(pl.multiple_of(r * 256, 256), 256)
            proj[u, at, :] = jnp.dot(
                tok[at, :], rhs, preferred_element_type=jnp.float32
            ).astype(jnp.bfloat16)
            return 0

        lax.fori_loop(0, 3, chunk, 0)

    def gate():
        gt[...] = jnp.zeros_like(gt)
        for yy in range(NY):
            for zz in range(NZ):
                k = (yy * NZ + zz) * 128
                gt[0:16, k : k + 128] = gb[yy, zz, 0] + gb[yy, zz, 1]
        logit = lax.dot_general(
            tok[...], gt[...], (((1,), (1,)), ((), ())), preferred_element_type=jnp.float32
        )
        logit = logit.T[0:8, :]
        soft = jnp.maximum(logit, 0.0) + jnp.log1p(jnp.exp(-jnp.abs(logit)))
        head = lax.broadcasted_iota(jnp.int32, (8, 128), 0)
        rate = jnp.zeros((8, 128), jnp.float32)
        for h in range(NH):
            rate = jnp.where(head == h, rate_ref[h], rate)
        decay = -rate[:, 0:1] * soft
        hi, mid, lo = thirds(decay)
        parts = jnp.concatenate([hi, mid, lo, jnp.zeros_like(lo)], axis=0).astype(jnp.bfloat16)
        before = lax.broadcasted_iota(jnp.int32, (768, 768), 0)
        after = lax.broadcasted_iota(jnp.int32, (768, 768), 1)
        upper = jnp.where(before <= after, 1.0, 0.0).astype(jnp.bfloat16)
        sums = jnp.dot(parts, upper, preferred_element_type=jnp.float32)
        within = sums[0:8] + sums[8:16] + sums[16:24]
        column = jnp.concatenate([within, jnp.zeros((120, 768), jnp.float32)], axis=0).T
        for h in range(NH):
            wrow[h] = jnp.broadcast_to(within[h : h + 1, :], (8, 768))
            wcol[h] = jnp.broadcast_to(column[:, h : h + 1], (768, 128))
            total[h] = jnp.broadcast_to(within[h : h + 1, 767:768], (8, 128))

    def half(k):
        return pl.ds(pl.multiple_of(k * 64, 64), 64)

    def local_state(u, h):
        key = proj[u, :, 0:128].astype(jnp.float32)
        scaled = (jnp.exp(total[h, 0:1, :] - wcol[h]) * key).astype(jnp.bfloat16)
        loc[h] = lax.dot_general(
            scaled, proj[u, :, 128:256], (((0,), (0,)), ((), ())),
            preferred_element_type=jnp.float32,
        )
        q, i = h // 2, lax.rem(h, 2)
        swap[q, 0, i, 0:64, :] = loc[h, half(1 - c), :]
        swap[q, 0, i, 64:72, :] = total[h]

    def swap_copy(q):
        return pltpu.make_async_remote_copy(
            src_ref=swap.at[q, 0], dst_ref=swap.at[q, 1], send_sem=swap_sem.at[q, 0],
            recv_sem=swap_sem.at[q, 1], device_id=mate, device_id_type=MESH,
        )

    def hand_copy(q, k):
        return pltpu.make_async_remote_copy(
            src_ref=hand.at[q], dst_ref=state.at[pl.ds(2 * q, 2), half(k)],
            send_sem=hand_sem.at[q, 0], recv_sem=hand_sem.at[q, 1],
            device_id=mate, device_id_type=MESH,
        )

    def all_z(q, d, src):
        ref = tz.at[q, lax.rem(src + NZ, NZ)]
        return pltpu.make_async_remote_copy(
            src_ref=ref, dst_ref=ref, send_sem=zs_sem.at[q], recv_sem=zr_sem.at[q, d - 1],
            device_id=seq_id(y, z + d, c), device_id_type=MESH,
        )

    def all_y(q, d, src):
        ref = ty.at[q, lax.rem(src + NY, NY)]
        return pltpu.make_async_remote_copy(
            src_ref=ref, dst_ref=ref, send_sem=ys_sem.at[q], recv_sem=yr_sem.at[q, d - 1],
            device_id=seq_id(y + d, z, c), device_id_type=MESH,
        )

    def x_ring(h):
        def item(i, p):
            return nb.at[h, i] if p is None else nb.at[h, i, pl.ds(p * 384, 384)]

        return Ring(item, NX, x, xp, xm, lambda i: xr_sem.at[h, i], xs_sem.at[h])

    def pack(ref, at, i, value, log):
        hi, mid, lo = thirds(log)
        row = lax.broadcasted_iota(jnp.int32, (16, 128), 0)
        tail = jnp.where(row == 0, hi, jnp.where(row == 1, mid, jnp.where(row == 2, lo, 0.0)))
        ref[at, i, 0:64, :] = value.astype(jnp.bfloat16)
        ref[at, i, 64:80, :] = tail.astype(jnp.bfloat16)

    def unpack(ref, at, i):
        tail = ref[at, i, 64:80, :].astype(jnp.float32)
        return ref[at, i, 0:64, :].astype(jnp.float32), jnp.sum(tail, axis=0, keepdims=True)

    def pair(q, i):
        h = 2 * q + i
        mine, theirs = loc[h, half(c), :], swap[q, 1, i, 0:64, :]
        own, other = total[h, 0:1, :], swap[q, 1, i, 64:65, :]
        first = c == 0
        return (
            jnp.where(first, mine, theirs), jnp.where(first, own, other),
            jnp.where(first, theirs, mine), jnp.where(first, other, own),
        )

    def below(ref, i, n, limit):
        acc_s = jnp.zeros((64, 128), jnp.float32)
        acc_a = jnp.zeros((1, 128), jnp.float32)
        kept = (acc_s, acc_a)
        for at in range(n):
            s_at, a_at = unpack(ref, at, i)
            acc_s, acc_a = jnp.exp(a_at) * acc_s + s_at, acc_a + a_at
            kept = tuple(
                jnp.where(at < limit, new, old) for new, old in zip((acc_s, acc_a), kept)
            )
        return kept, (acc_s, acc_a)

    def scan_step(k, q):
        if k == 1:
            swap_copy(q).wait_recv()
            for i in range(2):
                s0, a0, s1, a1 = pair(q, i)
                pack(tz.at[q], z, i, jnp.exp(a1) * s0 + s1, a0 + a1)
            for d in (4, 3, 5, 2, 6, 1, 7):
                all_z(q, d, z).start()
        elif k == 2:
            for d in range(1, NZ):
                all_z(q, d, z - d).wait_recv()
            for i in range(2):
                _, (row_s, row_a) = below(tz.at[q], i, NZ, z)
                pack(ty.at[q], y, i, row_s, row_a)
            for d in (2, 1, 3):
                all_y(q, d, y).start()
        elif k == 3:
            for d in range(1, NY):
                all_y(q, d, y - d).wait_recv()
            first = c == 0
            for i in range(2):
                (in_s, in_a), _ = below(tz.at[q], i, NZ, z)
                (row_s, _), _ = below(ty.at[q], i, NY, y)
                p0 = jnp.exp(in_a) * row_s + in_s
                s0, a0, _, _ = pair(q, i)
                p1 = jnp.exp(a0) * p0 + s0
                hand[q, i] = jnp.where(first, p1, p0).astype(jnp.bfloat16)
                state[2 * q + i, half(c), :] = jnp.where(first, p0, p1).astype(jnp.bfloat16)
            hand_copy(q, c).start()
        else:
            hand_copy(q, 1 - c).wait_recv()

    def attention(u, i, h):
        kv = h
        for r in range(3):
            lo, n = r * 256, (r + 1) * 256
            query = proj[u, lo:n, i * 128 : (i + 1) * 128]
            scores = lax.dot_general(
                query, proj[kv, 0:n, 0:128], (((1,), (1,)), ((), ())),
                preferred_element_type=jnp.float32,
            )
            col = wcol[h, lo:n, :]
            gap = jnp.concatenate([col] * (n // 128), axis=1) - wrow[h, 0:1, 0:n]
            t_at = lax.broadcasted_iota(jnp.int32, (256, n), 0) + lo
            s_at = lax.broadcasted_iota(jnp.int32, (256, n), 1)
            causal = s_at <= t_at
            attn = jnp.where(
                causal, scores * jnp.exp(jnp.where(causal, gap, 0.0)), 0.0
            ).astype(jnp.bfloat16)
            local[h, lo:n, :] = jnp.dot(
                attn, proj[kv, 0:n, 128:256], preferred_element_type=jnp.float32
            )
            qs[h, lo:n, :] = (jnp.exp(col) * query.astype(jnp.float32)).astype(jnp.bfloat16)

    def normed(h):
        out = local[h] + jnp.dot(qs[h], state[h], preferred_element_type=jnp.float32)
        scale = lax.rsqrt(jnp.mean(out * out, axis=-1, keepdims=True) + 1e-05)
        nb[h, x] = (out * scale * gain_ref[pl.ds(h, 1), :]).astype(jnp.bfloat16)
        x_ring(h).send(0)

    def mix(h, first, last):
        weight = ow[:, h].reshape(512, 1024)

        def chunk(r, _):
            at = pl.ds(pl.multiple_of(r * 256, 256), 256)
            lhs = jnp.concatenate([nb[h, i, at, :] for i in range(NX)], axis=1)
            part = jnp.dot(lhs, weight, preferred_element_type=jnp.float32)
            if not first:
                part = part + acc[at, :]
            if last:
                out_ref[at, :] = part.astype(jnp.bfloat16)
            else:
                acc[at, :] = part
            return 0

        lax.fori_loop(0, 3, chunk, 0)

    def slot(i, _):
        b = i - 3
        for k in (6, 4, 2, 0):
            valid(k, i - k // 2)

        @pl.when(i == 3)
        def _():
            pair_done(gb.at[:, :, 1 - c], NB).wait_recv()
            tok_load.wait()
            gate()

        @pl.when(i == 4)
        def _():
            scan_step(1, 0)

        @pl.when(i >= 3)
        def _():
            pair_done(w.at[pl.ds(2 * b, 2), :, :, :, 1 - c], b).wait_recv()
            project(2 * b)
            local_state(2 * b, 2 * b)

        for k in (5, 3, 1):
            valid(k, i - k // 2)

        @pl.when(i == 4)
        def _():
            scan_step(2, 0)

        @pl.when(i >= 3)
        def _():
            project(2 * b + 1)
            local_state(2 * b + 1, 2 * b + 1)
            swap_copy(b).start()

        return 0

    lax.fori_loop(0, 5, slot, 0)
    weight_round(6, NB - 1)
    scan_step(3, 0)
    scan_step(1, 1)
    pair_done(w.at[pl.ds(NU - 2, 2), :, :, :, 1 - c], NB - 1).wait_recv()
    project(4)

    def gathered(h):
        hop(x_ring(h), 2)
        mix(h, h == 0, h == NH - 1)

    attention(4, 0, 0)
    scan_step(4, 0)
    normed(0)
    attention(4, 1, 1)
    normed(1)
    scan_step(2, 1)
    project(5)
    scan_step(3, 1)
    hop(x_ring(0), 1)
    attention(5, 0, 2)
    scan_step(4, 1)
    normed(2)
    hop(x_ring(1), 1)
    attention(5, 1, 3)
    normed(3)
    ow_load.wait()
    gathered(0)
    hop(x_ring(2), 1)
    gathered(1)
    hop(x_ring(3), 1)
    gathered(2)
    gathered(3)
    finish()

    def end(h, _):
        sent(nb.at[h, pl.ds(0, 3)], xs_sem.at[h])
        return 0

    lax.fori_loop(0, NH, end, 0)
    for q in range(2):
        swap_copy(q).wait_send()
        sent(tz.at[q, pl.ds(0, 7)], zs_sem.at[q])
        sent(ty.at[q, pl.ds(0, 3)], ys_sem.at[q])
        hand_copy(q, c).wait_send()


def fused(tokens, wq, wk, wv, ow, gate, rate, gain):
    rows, depth = tokens.shape
    any_spec = pl.BlockSpec(memory_space=pl.ANY)
    vmem = pl.BlockSpec(memory_space=pltpu.VMEM)
    bf16, f32, dma = jnp.bfloat16, jnp.float32, pltpu.SemaphoreType.DMA
    return pl.pallas_call(
        kernel,
        out_shape=jax.ShapeDtypeStruct((rows, ow.shape[-1]), bf16),
        in_specs=[any_spec] * 5 + [vmem, pl.BlockSpec(memory_space=pltpu.SMEM), vmem],
        out_specs=vmem,
        scratch_shapes=[
            pltpu.VMEM((rows, depth), bf16),
            pltpu.VMEM((NU, 2, NY, NZ, 2, 64, 128), bf16),
            pltpu.VMEM((NY, NZ, 2, 16, 128), bf16),
            pltpu.VMEM((128, depth), bf16),
            pltpu.VMEM(ow.shape, bf16),
            pltpu.VMEM((NU, rows, 256), bf16),
            pltpu.VMEM((NH, rows, 128), f32),
            pltpu.VMEM((NH, 8, rows), f32),
            pltpu.VMEM((NH, 8, 128), f32),
            pltpu.VMEM((NH, 128, 128), f32),
            pltpu.VMEM((2, 2, 2, 72, 128), f32),
            pltpu.VMEM((2, NZ, 2, 80, 128), bf16),
            pltpu.VMEM((2, NY, 2, 80, 128), bf16),
            pltpu.VMEM((2, 2, 64, 128), bf16),
            pltpu.VMEM((NH, 128, 128), bf16),
            pltpu.VMEM((NH, rows, 128), f32),
            pltpu.VMEM((NH, rows, 128), bf16),
            pltpu.VMEM((NH, NX, rows, 128), bf16),
            pltpu.VMEM((rows, ow.shape[-1]), f32),
            dma((2 * NU + 3,)), dma((NB, 76)), dma((NB, 4)), dma((12,)), dma((2,)),
            dma((NB + 1,)), dma((NB + 1,)),
            dma((2, 2)), dma((2,)), dma((2, 8)), dma((2,)), dma((2, 4)), dma((2, 2)),
            dma((NH,)), dma((NH, 4)),
        ],
        compiler_params=pltpu.CompilerParams(
            collective_id=0, has_side_effects=True, vmem_limit_bytes=63 * 1024 * 1024
        ),
    )(tokens, wq, wk, wv, ow, gate, rate, gain)


def on_device(tokens, wq, wk, wv, wg, decay_rate, norm_gain, out_weight):
    ow = out_weight.reshape(NX, NH, 128, out_weight.shape[1])
    return fused(tokens, wq, wk, wv, ow, wg, decay_rate, norm_gain.reshape(NH, 128))


def solution(mesh):
    return jax.shard_map(
        on_device,
        mesh=mesh,
        in_specs=(
            P("seq", None), P("seq", "tp"), P("seq", "tp"), P("seq", "tp"), P("seq", "tp"),
            P("tp"), P("tp"), P(None, "tp"),
        ),
        out_specs=P("seq", "tp"),
        check_vma=False,
    )
```

```python
import jax
import jax.numpy as jnp
from jax import lax
from jax.experimental import pallas as pl
from jax.experimental.pallas import tpu as pltpu
from jax.sharding import PartitionSpec as P

NX, NY, NZ = 4, 4, 8
MESH = pl.DeviceIdType.MESH
UNITS = (
    ((1, 0), (2, 0)),
    ((1, 1), (2, 1)),
    ((1, 2), (2, 2)),
    ((1, 3), (2, 3)),
    ((0, 0), (0, 1)),
    ((0, 2), (0, 3)),
)
NU = len(UNITS)
NH = 4
NB = NU // 2
A1, A2, B1, B2 = 0, 4, 12, 20


class Ring:
    def __init__(self, item, n, pos, nxt, prv, recv, send, split=True):
        self.item, self.n, self.pos = item, n, pos
        self.nxt, self.prv, self.recv_sem, self.send_sem = nxt, prv, recv, send
        self.split = split

    def legs(self, r):
        last = r == self.n // 2 - 1
        parts = ((None, None), (0, 1))[last and self.split]
        dirs = (0,) if last and not self.split else (0, 1)
        return [(d, parts[d]) for d in dirs]

    def copy(self, idx, part, r, d):
        ref = self.item(lax.rem(idx + 2 * self.n, self.n), part)
        return pltpu.make_async_remote_copy(
            src_ref=ref,
            dst_ref=ref,
            send_sem=self.send_sem,
            recv_sem=self.recv_sem(2 * r + d),
            device_id=(self.nxt, self.prv)[d],
            device_id_type=MESH,
        )

    def send(self, r):
        for d, part in self.legs(r):
            self.copy(self.pos - r if d == 0 else self.pos + r, part, r, d).start()

    def recv(self, r):
        for d, part in self.legs(r):
            self.copy(
                self.pos - 1 - r if d == 0 else self.pos + 1 + r, part, r, d
            ).wait_recv()


class Direct:
    n = 2

    def __init__(self, item, pos, peers, recv, send):
        self.item, self.pos, self.peers = item, pos, peers
        self.recv_sem, self.send_sem = recv, send

    def copy(self, idx, d):
        ref = self.item(idx, None)
        return pltpu.make_async_remote_copy(
            src_ref=ref,
            dst_ref=ref,
            send_sem=self.send_sem,
            recv_sem=self.recv_sem(d - 1),
            device_id=self.peers[d - 1],
            device_id_type=MESH,
        )

    def send(self, r):
        for d in range(1, len(self.peers) + 1):
            self.copy(self.pos, d).start()

    def recv(self, r):
        for d in range(1, len(self.peers) + 1):
            self.copy(self.pos - d, d).wait_recv()


def thirds(v):
    hi = v.astype(jnp.bfloat16).astype(jnp.float32)
    mid = (v - hi).astype(jnp.bfloat16).astype(jnp.float32)
    return hi, mid, v - hi - mid


def kernel(
    tok_hbm, wq_hbm, wk_hbm, wv_hbm, ow_hbm, gate_ref, rate_ref, gain_ref,
    out_ref,
    tok, w, gb, gt, ow, proj, wcol, wrow, total, loc, swap, tz, ty, hand, state, local,
    qs, nb, acc,
    load_sem, recv_sem, send_sem, grecv_sem, gsend_sem, pair_send, pair_recv,
    swap_sem, zs_sem, zr_sem, ys_sem, yr_sem, hand_sem, xs_sem, xr_sem,
):
    x = lax.axis_index("tp")
    s = lax.axis_index("seq")
    y, z, c = s // (2 * NZ), lax.rem(s // 2, NZ), lax.rem(s, 2)

    def seq_id(yy, zz, cc):
        return {"seq": (lax.rem(yy + NY, NY) * NZ + lax.rem(zz + NZ, NZ)) * 2 + cc}

    yp, ym = seq_id(y + 1, z, c), seq_id(y - 1, z, c)
    zp, zm = seq_id(y, z + 1, c), seq_id(y, z - 1, c)
    mate = seq_id(y, z, 1 - c)
    y_peers = [seq_id(y + d, z, c) for d in range(1, NY)]
    z_peers = [seq_id(y, z + d, c) for d in range(1, NZ)]
    xp, xm = {"tp": lax.rem(x + 1, NX)}, {"tp": lax.rem(x + NX - 1, NX)}

    loads = []
    for u, tiles in enumerate(UNITS):
        for t, (m, h) in enumerate(tiles):
            src = (wq_hbm, wk_hbm, wv_hbm)[m].at[:, h * 128 : (h + 1) * 128]
            loads.append(
                pltpu.make_async_copy(src, w.at[u, t, y, z, c], load_sem.at[u * 2 + t])
            )
    for cp in loads:
        cp.start()
    tok_load = pltpu.make_async_copy(tok_hbm, tok, load_sem.at[2 * NU + 1])
    ow_load = pltpu.make_async_copy(ow_hbm, ow, load_sem.at[2 * NU + 2])

    barrier = pltpu.get_barrier_semaphore()
    partners = z_peers + y_peers + [mate, xp, xm]
    for dev in partners:
        pl.semaphore_signal(barrier, inc=1, device_id=dev, device_id_type=MESH)
    pl.semaphore_wait(barrier, len(partners))
    tok_load.start()
    ow_load.start()

    def rows(part):
        return slice(None) if part is None else pl.ds(part * 32, 32)

    def piece(b, tile, yy, zz, part):
        return w.at[pl.ds(2 * b, 2), tile, lax.rem(yy + NY, NY), lax.rem(zz + NZ, NZ), c, rows(part)]

    def rings(b):
        made = []
        base = 0

        def make(item, along_y, wait, k):
            nonlocal base
            first = base
            recv, send = lambda i: recv_sem.at[b, first + i], send_sem.at[b, k]
            if along_y:
                ring = Direct(item, y, y_peers, recv, send)
                base += NY - 1
            else:
                ring = Ring(item, NZ, z, zp, zm, recv, send)
                base += NZ
            made.append((wait, ring))

        make(lambda i, p: piece(b, 0, i, z, p), True, 0, 0)
        make(lambda i, p: piece(b, 1, y, i, p), False, 0, 1)
        for d in (0, 1, -1, 2):
            make(lambda i, p, d=d: piece(b, 0, y + d, i, p), False, min(abs(d), 1), 2)
        for d in (0, 1, -1, 2, -2, 3, -3, 4):
            make(lambda i, p, d=d: piece(b, 1, i, z + d, p), True, abs(d), 3)
        return made

    g1 = Direct(lambda i, p: gb.at[lax.rem(i + NY, NY), z, c], y, y_peers,
                lambda i: grecv_sem.at[i], gsend_sem.at[0])
    g2 = Direct(lambda i, p: gb.at[:, lax.rem(i + NZ, NZ), c], z, z_peers,
                lambda i: grecv_sem.at[4 + i], gsend_sem.at[1])

    def to_mate(ref, k):
        pltpu.make_async_remote_copy(
            src_ref=ref, dst_ref=ref, send_sem=pair_send.at[k], recv_sem=pair_recv.at[k],
            device_id=mate, device_id_type=MESH,
        ).start()

    def hop(ring, r):
        if r > 0:
            ring.recv(r - 1)
        if r < ring.n // 2:
            ring.send(r)

    def load_gate():
        k = lax.broadcasted_iota(jnp.int32, (64, 128), 0)
        lane = lax.broadcasted_iota(jnp.int32, (64, 128), 1)
        pick = jnp.where(lane == k + 64 * c, 1.0, 0.0).astype(jnp.bfloat16)
        turned = lax.dot_general(
            gate_ref[...], pick, (((1,), (0,)), ((), ())), preferred_element_type=jnp.float32
        )
        gb[y, z, c] = jnp.concatenate(
            [turned, jnp.zeros((12, 128), jnp.float32)], axis=0
        ).astype(jnp.bfloat16)

    def column(b, zz):
        to_mate(w.at[pl.ds(2 * b, 2), :, :, lax.rem(zz + NZ, NZ), c], b)

    def gate_round(k):
        if k == 0:
            g1.send(0)
        elif k == 1:
            g1.recv(0)
            g2.send(0)
            to_mate(g2.item(z, None), NB)
        else:
            g2.recv(0)
            for d in range(1, NZ):
                to_mate(g2.item(z - d, None), NB)

    def weight_round(k, b):
        if k == 0:
            for i in range(2):
                for t in range(2):
                    own = w.at[2 * b + i, t, y, z, c]
                    pltpu.make_async_copy(own, own, load_sem.at[b * 4 + 2 * i + t]).wait()

        todo = [(ring, k - wait) for wait, ring in rings(b)]
        for ring, r in todo:
            if 0 < r <= ring.n // 2:
                ring.recv(r - 1)
            if 0 <= r < ring.n // 2:
                ring.send(r)
        if k >= 1:
            d = k - 1
            for at in {0: (z,), 4: (z + 4,)}.get(d, (z + d, z - d)):
                column(b, at)

    def pair_done(ref, k):
        return pltpu.make_async_remote_copy(
            src_ref=ref, dst_ref=ref, send_sem=pair_send.at[k], recv_sem=pair_recv.at[k],
            device_id=mate, device_id_type=MESH,
        )

    def sent(ref, sem):
        pltpu.make_async_remote_copy(
            src_ref=ref, dst_ref=ref, send_sem=sem, recv_sem=pair_recv.at[0],
            device_id=mate, device_id_type=MESH,
        ).wait_send()

    def finish():
        pair_done(gb.at[:, :, c], NB).wait_send()
        sent(gb.at[pl.ds(0, 3), z, c], gsend_sem.at[0])
        sent(gb.at[:, pl.ds(0, 7), c], gsend_sem.at[1])

        def one(b, _):
            two = pl.ds(2 * b, 2)
            pair_done(w.at[two, :, :, :, c], b).wait_send()
            sent(w.at[two, 0, pl.ds(0, 3), z, c], send_sem.at[b, 0])
            sent(w.at[two, 1, y, pl.ds(0, 7), c], send_sem.at[b, 1])
            sent(w.at[two, 0, :, pl.ds(0, 7), c], send_sem.at[b, 2])
            sent(w.at[two, 1, pl.ds(0, 3), :, c], send_sem.at[b, 3])
            return 0

        lax.fori_loop(0, NB, one, 0)

    def project(u):
        rhs = jnp.concatenate(
            [w[u, 0].reshape(4096, 128), w[u, 1].reshape(4096, 128)], axis=1
        )

        def chunk(r, _):
            at = pl.ds(pl.multiple_of(r * 256, 256), 256)
            proj[u, at, :] = jnp.dot(
                tok[at, :], rhs, preferred_element_type=jnp.float32
            ).astype(jnp.bfloat16)
            return 0

        lax.fori_loop(0, 3, chunk, 0)

    def gate():
        gt[...] = jnp.zeros_like(gt)
        for yy in range(NY):
            for zz in range(NZ):
                k = (yy * NZ + zz) * 128
                gt[0:16, k : k + 128] = gb[yy, zz, 0] + gb[yy, zz, 1]
        logit = lax.dot_general(
            tok[...], gt[...], (((1,), (1,)), ((), ())), preferred_element_type=jnp.float32
        )
        logit = logit.T[0:8, :]
        soft = jnp.maximum(logit, 0.0) + jnp.log1p(jnp.exp(-jnp.abs(logit)))
        head = lax.broadcasted_iota(jnp.int32, (8, 128), 0)
        rate = jnp.zeros((8, 128), jnp.float32)
        for h in range(NH):
            rate = jnp.where(head == h, rate_ref[h], rate)
        decay = -rate[:, 0:1] * soft
        hi, mid, lo = thirds(decay)
        parts = jnp.concatenate([hi, mid, lo, jnp.zeros_like(lo)], axis=0).astype(jnp.bfloat16)
        before = lax.broadcasted_iota(jnp.int32, (768, 768), 0)
        after = lax.broadcasted_iota(jnp.int32, (768, 768), 1)
        upper = jnp.where(before <= after, 1.0, 0.0).astype(jnp.bfloat16)
        sums = jnp.dot(parts, upper, preferred_element_type=jnp.float32)
        within = sums[0:8] + sums[8:16] + sums[16:24]
        column = jnp.concatenate([within, jnp.zeros((120, 768), jnp.float32)], axis=0).T
        for h in range(NH):
            wrow[h] = jnp.broadcast_to(within[h : h + 1, :], (8, 768))
            wcol[h] = jnp.broadcast_to(column[:, h : h + 1], (768, 128))
            total[h] = jnp.broadcast_to(within[h : h + 1, 767:768], (8, 128))

    def half(k):
        return pl.ds(pl.multiple_of(k * 64, 64), 64)

    def local_state(u, h):
        key = proj[u, :, 0:128].astype(jnp.float32)
        scaled = (jnp.exp(total[h, 0:1, :] - wcol[h]) * key).astype(jnp.bfloat16)
        loc[h] = lax.dot_general(
            scaled, proj[u, :, 128:256], (((0,), (0,)), ((), ())),
            preferred_element_type=jnp.float32,
        )
        q, i = h // 2, lax.rem(h, 2)
        swap[q, 0, i, 0:64, :] = loc[h, half(1 - c), :]
        swap[q, 0, i, 64:72, :] = total[h]

    def swap_copy(q):
        return pltpu.make_async_remote_copy(
            src_ref=swap.at[q, 0], dst_ref=swap.at[q, 1], send_sem=swap_sem.at[q, 0],
            recv_sem=swap_sem.at[q, 1], device_id=mate, device_id_type=MESH,
        )

    def hand_copy(q, k):
        return pltpu.make_async_remote_copy(
            src_ref=hand.at[q], dst_ref=state.at[pl.ds(2 * q, 2), half(k)],
            send_sem=hand_sem.at[q, 0], recv_sem=hand_sem.at[q, 1],
            device_id=mate, device_id_type=MESH,
        )

    def all_z(q, d, src):
        ref = tz.at[q, lax.rem(src + NZ, NZ)]
        return pltpu.make_async_remote_copy(
            src_ref=ref, dst_ref=ref, send_sem=zs_sem.at[q], recv_sem=zr_sem.at[q, d - 1],
            device_id=seq_id(y, z + d, c), device_id_type=MESH,
        )

    def all_y(q, d, src):
        ref = ty.at[q, lax.rem(src + NY, NY)]
        return pltpu.make_async_remote_copy(
            src_ref=ref, dst_ref=ref, send_sem=ys_sem.at[q], recv_sem=yr_sem.at[q, d - 1],
            device_id=seq_id(y + d, z, c), device_id_type=MESH,
        )

    def x_ring(h):
        def item(i, p):
            return nb.at[h, i] if p is None else nb.at[h, i, pl.ds(p * 384, 384)]

        return Ring(item, NX, x, xp, xm, lambda i: xr_sem.at[h, i], xs_sem.at[h])

    def pack(ref, at, i, value, log):
        hi, mid, lo = thirds(log)
        row = lax.broadcasted_iota(jnp.int32, (16, 128), 0)
        tail = jnp.where(row == 0, hi, jnp.where(row == 1, mid, jnp.where(row == 2, lo, 0.0)))
        ref[at, i, 0:64, :] = value.astype(jnp.bfloat16)
        ref[at, i, 64:80, :] = tail.astype(jnp.bfloat16)

    def unpack(ref, at, i):
        tail = ref[at, i, 64:80, :].astype(jnp.float32)
        return ref[at, i, 0:64, :].astype(jnp.float32), jnp.sum(tail, axis=0, keepdims=True)

    def pair(q, i):
        h = 2 * q + i
        mine, theirs = loc[h, half(c), :], swap[q, 1, i, 0:64, :]
        own, other = total[h, 0:1, :], swap[q, 1, i, 64:65, :]
        first = c == 0
        return (
            jnp.where(first, mine, theirs), jnp.where(first, own, other),
            jnp.where(first, theirs, mine), jnp.where(first, other, own),
        )

    def below(ref, i, n, limit):
        acc_s = jnp.zeros((64, 128), jnp.float32)
        acc_a = jnp.zeros((1, 128), jnp.float32)
        kept = (acc_s, acc_a)
        for at in range(n):
            s_at, a_at = unpack(ref, at, i)
            acc_s, acc_a = jnp.exp(a_at) * acc_s + s_at, acc_a + a_at
            kept = tuple(
                jnp.where(at < limit, new, old) for new, old in zip((acc_s, acc_a), kept)
            )
        return kept, (acc_s, acc_a)

    def scan_step(k, q):
        if k == 1:
            swap_copy(q).wait_recv()
            for i in range(2):
                s0, a0, s1, a1 = pair(q, i)
                pack(tz.at[q], z, i, jnp.exp(a1) * s0 + s1, a0 + a1)
            for d in (4, 3, 5, 2, 6, 1, 7):
                all_z(q, d, z).start()
        elif k == 2:
            for d in range(1, NZ):
                all_z(q, d, z - d).wait_recv()
            for i in range(2):
                _, (row_s, row_a) = below(tz.at[q], i, NZ, z)
                pack(ty.at[q], y, i, row_s, row_a)
            for d in (2, 1, 3):
                all_y(q, d, y).start()
        elif k == 3:
            for d in range(1, NY):
                all_y(q, d, y - d).wait_recv()
            first = c == 0
            for i in range(2):
                (in_s, in_a), _ = below(tz.at[q], i, NZ, z)
                (row_s, _), _ = below(ty.at[q], i, NY, y)
                p0 = jnp.exp(in_a) * row_s + in_s
                s0, a0, _, _ = pair(q, i)
                p1 = jnp.exp(a0) * p0 + s0
                hand[q, i] = jnp.where(first, p1, p0).astype(jnp.bfloat16)
                state[2 * q + i, half(c), :] = jnp.where(first, p0, p1).astype(jnp.bfloat16)
            hand_copy(q, c).start()
        else:
            hand_copy(q, 1 - c).wait_recv()

    def attention(u, i, h):
        kv = h
        for r in range(3):
            lo, n = r * 256, (r + 1) * 256
            query = proj[u, lo:n, i * 128 : (i + 1) * 128]
            scores = lax.dot_general(
                query, proj[kv, 0:n, 0:128], (((1,), (1,)), ((), ())),
                preferred_element_type=jnp.float32,
            )
            col = wcol[h, lo:n, :]
            gap = jnp.concatenate([col] * (n // 128), axis=1) - wrow[h, 0:1, 0:n]
            t_at = lax.broadcasted_iota(jnp.int32, (256, n), 0) + lo
            s_at = lax.broadcasted_iota(jnp.int32, (256, n), 1)
            causal = s_at <= t_at
            attn = jnp.where(
                causal, scores * jnp.exp(jnp.where(causal, gap, 0.0)), 0.0
            ).astype(jnp.bfloat16)
            local[h, lo:n, :] = jnp.dot(
                attn, proj[kv, 0:n, 128:256], preferred_element_type=jnp.float32
            )
            qs[h, lo:n, :] = (jnp.exp(col) * query.astype(jnp.float32)).astype(jnp.bfloat16)

    def normed(h):
        out = local[h] + jnp.dot(qs[h], state[h], preferred_element_type=jnp.float32)
        scale = lax.rsqrt(jnp.mean(out * out, axis=-1, keepdims=True) + 1e-05)
        nb[h, x] = (out * scale * gain_ref[pl.ds(h, 1), :]).astype(jnp.bfloat16)
        x_ring(h).send(0)

    def mix(h, first, last):
        weight = ow[:, h].reshape(512, 1024)

        def chunk(r, _):
            at = pl.ds(pl.multiple_of(r * 256, 256), 256)
            lhs = jnp.concatenate([nb[h, i, at, :] for i in range(NX)], axis=1)
            part = jnp.dot(lhs, weight, preferred_element_type=jnp.float32)
            if not first:
                part = part + acc[at, :]
            if last:
                out_ref[at, :] = part.astype(jnp.bfloat16)
            else:
                acc[at, :] = part
            return 0

        lax.fori_loop(0, 3, chunk, 0)

    def arrived(b):
        pair_done(w.at[pl.ds(2 * b, 2), :, :, :, 1 - c], b).wait_recv()

    def key_value(u):
        project(u)
        local_state(u, u)

    def slot(t, _):
        for k in range(5, -1, -1):
            @pl.when((t >= k) & (t < k + NB))
            def _():
                weight_round(k, t - k)

        for k in range(3):
            pl.when(t == k)(lambda k=k: gate_round(k))

        @pl.when(t == 3)
        def _():
            pair_done(gb.at[:, :, 1 - c], NB).wait_recv()
            tok_load.wait()
            gate()

        @pl.when(t == 6)
        def _():
            scan_step(1, 0)

        @pl.when(t >= 5)
        def _():
            b = t - 5
            arrived(b)
            key_value(2 * b)
            key_value(2 * b + 1)
            swap_copy(b).start()

        return 0

    def gathered(h):
        hop(x_ring(h), 2)
        mix(h, h == 0, h == NH - 1)

    load_gate()
    lax.fori_loop(0, 7, slot, 0)
    weight_round(5, NB - 1)
    scan_step(2, 0)
    scan_step(1, 1)
    arrived(2)
    project(4)
    scan_step(3, 0)
    attention(4, 0, 0)
    scan_step(4, 0)
    normed(0)
    attention(4, 1, 1)
    normed(1)
    scan_step(2, 1)
    project(5)
    scan_step(3, 1)
    hop(x_ring(0), 1)
    attention(5, 0, 2)
    scan_step(4, 1)
    normed(2)
    hop(x_ring(1), 1)
    attention(5, 1, 3)
    normed(3)
    ow_load.wait()
    gathered(0)
    hop(x_ring(2), 1)
    gathered(1)
    hop(x_ring(3), 1)
    gathered(2)
    gathered(3)
    finish()

    def end(h, _):
        sent(nb.at[h, pl.ds(0, 3)], xs_sem.at[h])
        return 0

    lax.fori_loop(0, NH, end, 0)
    for q in range(2):
        swap_copy(q).wait_send()
        sent(tz.at[q, pl.ds(0, 7)], zs_sem.at[q])
        sent(ty.at[q, pl.ds(0, 3)], ys_sem.at[q])
        hand_copy(q, c).wait_send()


def fused(tokens, wq, wk, wv, ow, gate, rate, gain):
    rows, depth = tokens.shape
    any_spec = pl.BlockSpec(memory_space=pl.ANY)
    vmem = pl.BlockSpec(memory_space=pltpu.VMEM)
    bf16, f32, dma = jnp.bfloat16, jnp.float32, pltpu.SemaphoreType.DMA
    return pl.pallas_call(
        kernel,
        out_shape=jax.ShapeDtypeStruct((rows, ow.shape[-1]), bf16),
        in_specs=[any_spec] * 5 + [vmem, pl.BlockSpec(memory_space=pltpu.SMEM), vmem],
        out_specs=vmem,
        scratch_shapes=[
            pltpu.VMEM((rows, depth), bf16),
            pltpu.VMEM((NU, 2, NY, NZ, 2, 64, 128), bf16),
            pltpu.VMEM((NY, NZ, 2, 16, 128), bf16),
            pltpu.VMEM((128, depth), bf16),
            pltpu.VMEM(ow.shape, bf16),
            pltpu.VMEM((NU, rows, 256), bf16),
            pltpu.VMEM((NH, rows, 128), f32),
            pltpu.VMEM((NH, 8, rows), f32),
            pltpu.VMEM((NH, 8, 128), f32),
            pltpu.VMEM((NH, 128, 128), f32),
            pltpu.VMEM((2, 2, 2, 72, 128), f32),
            pltpu.VMEM((2, NZ, 2, 80, 128), bf16),
            pltpu.VMEM((2, NY, 2, 80, 128), bf16),
            pltpu.VMEM((2, 2, 64, 128), bf16),
            pltpu.VMEM((NH, 128, 128), bf16),
            pltpu.VMEM((NH, rows, 128), f32),
            pltpu.VMEM((NH, rows, 128), bf16),
            pltpu.VMEM((NH, NX, rows, 128), bf16),
            pltpu.VMEM((rows, ow.shape[-1]), f32),
            dma((2 * NU + 3,)), dma((NB, 67)), dma((NB, 4)), dma((12,)), dma((2,)),
            dma((NB + 1,)), dma((NB + 1,)),
            dma((2, 2)), dma((2,)), dma((2, 8)), dma((2,)), dma((2, 4)), dma((2, 2)),
            dma((NH,)), dma((NH, 4)),
        ],
        compiler_params=pltpu.CompilerParams(
            collective_id=0, has_side_effects=True, vmem_limit_bytes=63 * 1024 * 1024
        ),
    )(tokens, wq, wk, wv, ow, gate, rate, gain)


def on_device(tokens, wq, wk, wv, wg, decay_rate, norm_gain, out_weight):
    ow = out_weight.reshape(NX, NH, 128, out_weight.shape[1])
    return fused(tokens, wq, wk, wv, ow, wg.T, decay_rate, norm_gain.reshape(NH, 128))


def solution(mesh):
    return jax.shard_map(
        on_device,
        mesh=mesh,
        in_specs=(
            P("seq", None), P("seq", "tp"), P("seq", "tp"), P("seq", "tp"), P("seq", "tp"),
            P("tp"), P("tp"), P(None, "tp"),
        ),
        out_specs=P("seq", "tp"),
        check_vma=False,
    )
```

```python
import jax
import jax.numpy as jnp
from jax import lax
from jax.experimental import pallas as pl
from jax.experimental.pallas import tpu as pltpu
from jax.sharding import PartitionSpec as P

NX, NY, NZ = 4, 4, 8
MESH = pl.DeviceIdType.MESH
UNITS = (
    ((1, 0), (2, 0)),
    ((1, 1), (2, 1)),
    ((1, 2), (2, 2)),
    ((1, 3), (2, 3)),
    ((0, 0), (0, 1)),
    ((0, 2), (0, 3)),
)
NU = len(UNITS)
NH = 4
NB = NU // 2
A1, A2, B1, B2 = 0, 4, 12, 20


class Ring:
    def __init__(self, item, n, pos, nxt, prv, recv, send, split=True):
        self.item, self.n, self.pos = item, n, pos
        self.nxt, self.prv, self.recv_sem, self.send_sem = nxt, prv, recv, send
        self.split = split

    def legs(self, r):
        last = r == self.n // 2 - 1
        parts = ((None, None), (0, 1))[last and self.split]
        dirs = (0,) if last and not self.split else (0, 1)
        return [(d, parts[d]) for d in dirs]

    def copy(self, idx, part, r, d):
        ref = self.item(lax.rem(idx + 2 * self.n, self.n), part)
        return pltpu.make_async_remote_copy(
            src_ref=ref,
            dst_ref=ref,
            send_sem=self.send_sem,
            recv_sem=self.recv_sem(2 * r + d),
            device_id=(self.nxt, self.prv)[d],
            device_id_type=MESH,
        )

    def send(self, r):
        for d, part in self.legs(r):
            self.copy(self.pos - r if d == 0 else self.pos + r, part, r, d).start()

    def recv(self, r):
        for d, part in self.legs(r):
            self.copy(
                self.pos - 1 - r if d == 0 else self.pos + 1 + r, part, r, d
            ).wait_recv()


class Direct:
    n = 2

    def __init__(self, item, pos, peers, recv, send):
        self.item, self.pos, self.peers = item, pos, peers
        self.recv_sem, self.send_sem = recv, send

    def copy(self, idx, d):
        ref = self.item(idx, None)
        return pltpu.make_async_remote_copy(
            src_ref=ref,
            dst_ref=ref,
            send_sem=self.send_sem,
            recv_sem=self.recv_sem(d - 1),
            device_id=self.peers[d - 1],
            device_id_type=MESH,
        )

    def send(self, r):
        for d in range(1, len(self.peers) + 1):
            self.copy(self.pos, d).start()

    def recv(self, r):
        for d in range(1, len(self.peers) + 1):
            self.copy(self.pos - d, d).wait_recv()


def thirds(v):
    hi = v.astype(jnp.bfloat16).astype(jnp.float32)
    mid = (v - hi).astype(jnp.bfloat16).astype(jnp.float32)
    return hi, mid, v - hi - mid


def kernel(
    tok_hbm, wq_hbm, wk_hbm, wv_hbm, ow_hbm, gate_ref, rate_ref, gain_ref,
    out_ref,
    tok, w, gb, gt, ow, proj, wcol, wrow, total, loc, swap, tz, ty, hand, state, local,
    qs, nb, acc,
    load_sem, recv_sem, send_sem, grecv_sem, gsend_sem, pair_send, pair_recv,
    swap_sem, zs_sem, zr_sem, ys_sem, yr_sem, hand_sem, xs_sem, xr_sem,
):
    x = lax.axis_index("tp")
    s = lax.axis_index("seq")
    y, z, c = s // (2 * NZ), lax.rem(s // 2, NZ), lax.rem(s, 2)

    def seq_id(yy, zz, cc):
        return {"seq": (lax.rem(yy + NY, NY) * NZ + lax.rem(zz + NZ, NZ)) * 2 + cc}

    yp, ym = seq_id(y + 1, z, c), seq_id(y - 1, z, c)
    zp, zm = seq_id(y, z + 1, c), seq_id(y, z - 1, c)
    mate = seq_id(y, z, 1 - c)
    y_peers = [seq_id(y + d, z, c) for d in range(1, NY)]
    z_peers = [seq_id(y, z + d, c) for d in range(1, NZ)]
    xp, xm = {"tp": lax.rem(x + 1, NX)}, {"tp": lax.rem(x + NX - 1, NX)}

    loads = []
    for u, tiles in enumerate(UNITS):
        for t, (m, h) in enumerate(tiles):
            src = (wq_hbm, wk_hbm, wv_hbm)[m].at[:, h * 128 : (h + 1) * 128]
            loads.append(
                pltpu.make_async_copy(src, w.at[u, t, y, z, c], load_sem.at[u * 2 + t])
            )
    for cp in loads:
        cp.start()
    tok_load = pltpu.make_async_copy(tok_hbm, tok, load_sem.at[2 * NU + 1])
    ow_load = pltpu.make_async_copy(ow_hbm, ow, load_sem.at[2 * NU + 2])

    barrier = pltpu.get_barrier_semaphore()
    partners = z_peers + y_peers + [mate, xp, xm]
    for dev in partners:
        pl.semaphore_signal(barrier, inc=1, device_id=dev, device_id_type=MESH)
    pl.semaphore_wait(barrier, len(partners))
    tok_load.start()
    ow_load.start()

    def rows(part):
        return slice(None) if part is None else pl.ds(part * 32, 32)

    def piece(b, tile, yy, zz, part):
        return w.at[pl.ds(2 * b, 2), tile, lax.rem(yy + NY, NY), lax.rem(zz + NZ, NZ), c, rows(part)]

    def rings(b):
        made = []
        base = 0

        def make(item, along_y, wait, k):
            nonlocal base
            first = base
            recv, send = lambda i: recv_sem.at[b, first + i], send_sem.at[b, k]
            if along_y:
                ring = Direct(item, y, y_peers, recv, send)
                base += NY - 1
            else:
                ring = Ring(item, NZ, z, zp, zm, recv, send)
                base += NZ
            made.append((wait, ring))

        make(lambda i, p: piece(b, 0, i, z, p), True, 0, 0)
        make(lambda i, p: piece(b, 1, y, i, p), False, 0, 1)
        for d in (0, 1, -1, 2):
            make(lambda i, p, d=d: piece(b, 0, y + d, i, p), False, min(abs(d), 1), 2)
        for d in (0, 1, -1, 2, -2, 3, -3, 4):
            make(lambda i, p, d=d: piece(b, 1, i, z + d, p), True, abs(d), 3)
        return made

    g1 = Direct(lambda i, p: gb.at[lax.rem(i + NY, NY), z, c], y, y_peers,
                lambda i: grecv_sem.at[i], gsend_sem.at[0])
    g2 = Direct(lambda i, p: gb.at[:, lax.rem(i + NZ, NZ), c], z, z_peers,
                lambda i: grecv_sem.at[4 + i], gsend_sem.at[1])

    def to_mate(ref, k):
        pltpu.make_async_remote_copy(
            src_ref=ref, dst_ref=ref, send_sem=pair_send.at[k], recv_sem=pair_recv.at[k],
            device_id=mate, device_id_type=MESH,
        ).start()

    def hop(ring, r):
        if r > 0:
            ring.recv(r - 1)
        if r < ring.n // 2:
            ring.send(r)

    def load_gate():
        k = lax.broadcasted_iota(jnp.int32, (64, 128), 0)
        lane = lax.broadcasted_iota(jnp.int32, (64, 128), 1)
        pick = jnp.where(lane == k + 64 * c, 1.0, 0.0).astype(jnp.bfloat16)
        turned = lax.dot_general(
            gate_ref[...], pick, (((1,), (0,)), ((), ())), preferred_element_type=jnp.float32
        )
        gb[y, z, c] = jnp.concatenate(
            [turned, jnp.zeros((12, 128), jnp.float32)], axis=0
        ).astype(jnp.bfloat16)

    def column(b, zz):
        to_mate(w.at[pl.ds(2 * b, 2), :, :, lax.rem(zz + NZ, NZ), c], b)

    def gate_round(k):
        if k == 0:
            g1.send(0)
        elif k == 1:
            g1.recv(0)
            g2.send(0)
            to_mate(g2.item(z, None), NB)
        else:
            g2.recv(0)
            for d in range(1, NZ):
                to_mate(g2.item(z - d, None), NB)

    def weight_round(k, b):
        if k == 0:
            for i in range(2):
                for t in range(2):
                    own = w.at[2 * b + i, t, y, z, c]
                    pltpu.make_async_copy(own, own, load_sem.at[b * 4 + 2 * i + t]).wait()

        todo = [(ring, k - wait) for wait, ring in rings(b)]
        for ring, r in todo:
            if 0 < r <= ring.n // 2:
                ring.recv(r - 1)
            if 0 <= r < ring.n // 2:
                ring.send(r)
        if k >= 1:
            d = k - 1
            for at in {0: (z,), 4: (z + 4,)}.get(d, (z + d, z - d)):
                column(b, at)

    def pair_done(ref, k):
        return pltpu.make_async_remote_copy(
            src_ref=ref, dst_ref=ref, send_sem=pair_send.at[k], recv_sem=pair_recv.at[k],
            device_id=mate, device_id_type=MESH,
        )

    def sent(ref, sem):
        pltpu.make_async_remote_copy(
            src_ref=ref, dst_ref=ref, send_sem=sem, recv_sem=pair_recv.at[0],
            device_id=mate, device_id_type=MESH,
        ).wait_send()

    def finish():
        pair_done(gb.at[:, :, c], NB).wait_send()
        sent(gb.at[pl.ds(0, 3), z, c], gsend_sem.at[0])
        sent(gb.at[:, pl.ds(0, 7), c], gsend_sem.at[1])

        def one(b, _):
            two = pl.ds(2 * b, 2)
            pair_done(w.at[two, :, :, :, c], b).wait_send()
            sent(w.at[two, 0, pl.ds(0, 3), z, c], send_sem.at[b, 0])
            sent(w.at[two, 1, y, pl.ds(0, 7), c], send_sem.at[b, 1])
            sent(w.at[two, 0, :, pl.ds(0, 7), c], send_sem.at[b, 2])
            sent(w.at[two, 1, pl.ds(0, 3), :, c], send_sem.at[b, 3])
            return 0

        lax.fori_loop(0, NB, one, 0)

    def project(u):
        rhs = jnp.concatenate(
            [w[u, 0].reshape(4096, 128), w[u, 1].reshape(4096, 128)], axis=1
        )

        def chunk(r, _):
            at = pl.ds(pl.multiple_of(r * 256, 256), 256)
            proj[u, at, :] = jnp.dot(
                tok[at, :], rhs, preferred_element_type=jnp.float32
            ).astype(jnp.bfloat16)
            return 0

        lax.fori_loop(0, 3, chunk, 0)

    def gate():
        gt[...] = jnp.zeros_like(gt)
        for yy in range(NY):
            for zz in range(NZ):
                k = (yy * NZ + zz) * 128
                gt[0:16, k : k + 128] = gb[yy, zz, 0] + gb[yy, zz, 1]
        logit = lax.dot_general(
            tok[...], gt[...], (((1,), (1,)), ((), ())), preferred_element_type=jnp.float32
        )
        logit = logit.T[0:8, :]
        soft = jnp.maximum(logit, 0.0) + jnp.log1p(jnp.exp(-jnp.abs(logit)))
        head = lax.broadcasted_iota(jnp.int32, (8, 128), 0)
        rate = jnp.zeros((8, 128), jnp.float32)
        for h in range(NH):
            rate = jnp.where(head == h, rate_ref[h], rate)
        decay = -rate[:, 0:1] * soft
        hi, mid, lo = thirds(decay)
        parts = jnp.concatenate([hi, mid, lo, jnp.zeros_like(lo)], axis=0).astype(jnp.bfloat16)
        before = lax.broadcasted_iota(jnp.int32, (768, 768), 0)
        after = lax.broadcasted_iota(jnp.int32, (768, 768), 1)
        upper = jnp.where(before <= after, 1.0, 0.0).astype(jnp.bfloat16)
        sums = jnp.dot(parts, upper, preferred_element_type=jnp.float32)
        within = sums[0:8] + sums[8:16] + sums[16:24]
        column = jnp.concatenate([within, jnp.zeros((120, 768), jnp.float32)], axis=0).T
        for h in range(NH):
            wrow[h] = jnp.broadcast_to(within[h : h + 1, :], (8, 768))
            wcol[h] = jnp.broadcast_to(column[:, h : h + 1], (768, 128))
            total[h] = jnp.broadcast_to(within[h : h + 1, 767:768], (8, 128))

    def half(k):
        return pl.ds(pl.multiple_of(k * 64, 64), 64)

    def local_state(u, h):
        key = proj[u, :, 0:128].astype(jnp.float32)
        scaled = (jnp.exp(total[h, 0:1, :] - wcol[h]) * key).astype(jnp.bfloat16)
        loc[h] = lax.dot_general(
            scaled, proj[u, :, 128:256], (((0,), (0,)), ((), ())),
            preferred_element_type=jnp.float32,
        )
        q, i = h // 2, lax.rem(h, 2)
        swap[q, 0, i, 0:64, :] = loc[h, half(1 - c), :]
        swap[q, 0, i, 64:72, :] = total[h]

    def swap_copy(q):
        return pltpu.make_async_remote_copy(
            src_ref=swap.at[q, 0], dst_ref=swap.at[q, 1], send_sem=swap_sem.at[q, 0],
            recv_sem=swap_sem.at[q, 1], device_id=mate, device_id_type=MESH,
        )

    def hand_copy(q, k):
        return pltpu.make_async_remote_copy(
            src_ref=hand.at[q], dst_ref=state.at[pl.ds(2 * q, 2), half(k)],
            send_sem=hand_sem.at[q, 0], recv_sem=hand_sem.at[q, 1],
            device_id=mate, device_id_type=MESH,
        )

    def all_z(q, d, src):
        ref = tz.at[q, lax.rem(src + NZ, NZ)]
        return pltpu.make_async_remote_copy(
            src_ref=ref, dst_ref=ref, send_sem=zs_sem.at[q], recv_sem=zr_sem.at[q, d - 1],
            device_id=seq_id(y, z + d, c), device_id_type=MESH,
        )

    def all_y(q, d, src):
        ref = ty.at[q, lax.rem(src + NY, NY)]
        return pltpu.make_async_remote_copy(
            src_ref=ref, dst_ref=ref, send_sem=ys_sem.at[q], recv_sem=yr_sem.at[q, d - 1],
            device_id=seq_id(y + d, z, c), device_id_type=MESH,
        )

    def x_ring(h):
        def item(i, p):
            return nb.at[h, i] if p is None else nb.at[h, i, pl.ds(p * 384, 384)]

        return Ring(item, NX, x, xp, xm, lambda i: xr_sem.at[h, i], xs_sem.at[h])

    def pack(ref, at, i, value, log):
        hi, mid, lo = thirds(log)
        row = lax.broadcasted_iota(jnp.int32, (16, 128), 0)
        tail = jnp.where(row == 0, hi, jnp.where(row == 1, mid, jnp.where(row == 2, lo, 0.0)))
        ref[at, i, 0:64, :] = value.astype(jnp.bfloat16)
        ref[at, i, 64:80, :] = tail.astype(jnp.bfloat16)

    def unpack(ref, at, i):
        tail = ref[at, i, 64:80, :].astype(jnp.float32)
        return ref[at, i, 0:64, :].astype(jnp.float32), jnp.sum(tail, axis=0, keepdims=True)

    def pair(q, i):
        h = 2 * q + i
        mine, theirs = loc[h, half(c), :], swap[q, 1, i, 0:64, :]
        own, other = total[h, 0:1, :], swap[q, 1, i, 64:65, :]
        first = c == 0
        return (
            jnp.where(first, mine, theirs), jnp.where(first, own, other),
            jnp.where(first, theirs, mine), jnp.where(first, other, own),
        )

    def below(ref, i, n, limit):
        acc_s = jnp.zeros((64, 128), jnp.float32)
        acc_a = jnp.zeros((1, 128), jnp.float32)
        kept = (acc_s, acc_a)
        for at in range(n):
            s_at, a_at = unpack(ref, at, i)
            acc_s, acc_a = jnp.exp(a_at) * acc_s + s_at, acc_a + a_at
            kept = tuple(
                jnp.where(at < limit, new, old) for new, old in zip((acc_s, acc_a), kept)
            )
        return kept, (acc_s, acc_a)

    def scan_step(k, q):
        if k == 1:
            swap_copy(q).wait_recv()
            for i in range(2):
                s0, a0, s1, a1 = pair(q, i)
                pack(tz.at[q], z, i, jnp.exp(a1) * s0 + s1, a0 + a1)
            for d in (4, 3, 5, 2, 6, 1, 7):
                all_z(q, d, z).start()
        elif k == 2:
            for d in range(1, NZ):
                all_z(q, d, z - d).wait_recv()
            for i in range(2):
                _, (row_s, row_a) = below(tz.at[q], i, NZ, z)
                pack(ty.at[q], y, i, row_s, row_a)
            for d in (2, 1, 3):
                all_y(q, d, y).start()
        elif k == 3:
            for d in range(1, NY):
                all_y(q, d, y - d).wait_recv()
            first = c == 0
            for i in range(2):
                (in_s, in_a), _ = below(tz.at[q], i, NZ, z)
                (row_s, _), _ = below(ty.at[q], i, NY, y)
                p0 = jnp.exp(in_a) * row_s + in_s
                s0, a0, _, _ = pair(q, i)
                p1 = jnp.exp(a0) * p0 + s0
                hand[q, i] = jnp.where(first, p1, p0).astype(jnp.bfloat16)
                state[2 * q + i, half(c), :] = jnp.where(first, p0, p1).astype(jnp.bfloat16)
            hand_copy(q, c).start()
        else:
            hand_copy(q, 1 - c).wait_recv()

    def attention(u, i, h):
        kv = h
        for r in range(3):
            lo, n = r * 256, (r + 1) * 256
            query = proj[u, lo:n, i * 128 : (i + 1) * 128]
            scores = lax.dot_general(
                query, proj[kv, 0:n, 0:128], (((1,), (1,)), ((), ())),
                preferred_element_type=jnp.float32,
            )
            col = wcol[h, lo:n, :]
            gap = jnp.concatenate([col] * (n // 128), axis=1) - wrow[h, 0:1, 0:n]
            t_at = lax.broadcasted_iota(jnp.int32, (256, n), 0) + lo
            s_at = lax.broadcasted_iota(jnp.int32, (256, n), 1)
            causal = s_at <= t_at
            attn = jnp.where(
                causal, scores * jnp.exp(jnp.where(causal, gap, 0.0)), 0.0
            ).astype(jnp.bfloat16)
            local[h, lo:n, :] = jnp.dot(
                attn, proj[kv, 0:n, 128:256], preferred_element_type=jnp.float32
            )
            qs[h, lo:n, :] = (jnp.exp(col) * query.astype(jnp.float32)).astype(jnp.bfloat16)

    def normed(h):
        out = local[h] + jnp.dot(qs[h], state[h], preferred_element_type=jnp.float32)
        scale = lax.rsqrt(jnp.mean(out * out, axis=-1, keepdims=True) + 1e-05)
        nb[h, x] = (out * scale * gain_ref[pl.ds(h, 1), :]).astype(jnp.bfloat16)
        x_ring(h).send(0)

    def mix(h, first, last):
        weight = ow[:, h].reshape(512, 1024)

        def chunk(r, _):
            at = pl.ds(pl.multiple_of(r * 256, 256), 256)
            lhs = jnp.concatenate([nb[h, i, at, :] for i in range(NX)], axis=1)
            part = jnp.dot(lhs, weight, preferred_element_type=jnp.float32)
            if not first:
                part = part + acc[at, :]
            if last:
                out_ref[at, :] = part.astype(jnp.bfloat16)
            else:
                acc[at, :] = part
            return 0

        lax.fori_loop(0, 3, chunk, 0)

    def arrived(b):
        pair_done(w.at[pl.ds(2 * b, 2), :, :, :, 1 - c], b).wait_recv()

    def key_value(u):
        project(u)
        local_state(u, u)

    def slot(t, _):
        for k in range(5, -1, -1):
            @pl.when((t >= k) & (t < k + NB))
            def _():
                weight_round(k, t - k)

        for k in range(3):
            pl.when(t == k)(lambda k=k: gate_round(k))

        @pl.when(t == 3)
        def _():
            pair_done(gb.at[:, :, 1 - c], NB).wait_recv()
            tok_load.wait()
            gate()

        @pl.when(t == 6)
        def _():
            scan_step(1, 0)

        @pl.when(t >= 5)
        def _():
            b = t - 5
            arrived(b)
            key_value(2 * b)
            key_value(2 * b + 1)
            swap_copy(b).start()

        return 0

    def gathered(h):
        hop(x_ring(h), 2)
        mix(h, h == 0, h == NH - 1)

    load_gate()
    lax.fori_loop(0, 7, slot, 0)
    scan_step(2, 0)
    scan_step(1, 1)
    weight_round(5, NB - 1)
    scan_step(3, 0)
    arrived(2)
    project(4)
    attention(4, 0, 0)
    scan_step(4, 0)
    normed(0)
    attention(4, 1, 1)
    normed(1)
    scan_step(2, 1)
    project(5)
    scan_step(3, 1)
    hop(x_ring(0), 1)
    attention(5, 0, 2)
    scan_step(4, 1)
    normed(2)
    hop(x_ring(1), 1)
    attention(5, 1, 3)
    normed(3)
    ow_load.wait()
    gathered(0)
    hop(x_ring(2), 1)
    gathered(1)
    hop(x_ring(3), 1)
    gathered(2)
    gathered(3)
    finish()

    def end(h, _):
        sent(nb.at[h, pl.ds(0, 3)], xs_sem.at[h])
        return 0

    lax.fori_loop(0, NH, end, 0)
    for q in range(2):
        swap_copy(q).wait_send()
        sent(tz.at[q, pl.ds(0, 7)], zs_sem.at[q])
        sent(ty.at[q, pl.ds(0, 3)], ys_sem.at[q])
        hand_copy(q, c).wait_send()


def fused(tokens, wq, wk, wv, ow, gate, rate, gain):
    rows, depth = tokens.shape
    any_spec = pl.BlockSpec(memory_space=pl.ANY)
    vmem = pl.BlockSpec(memory_space=pltpu.VMEM)
    bf16, f32, dma = jnp.bfloat16, jnp.float32, pltpu.SemaphoreType.DMA
    return pl.pallas_call(
        kernel,
        out_shape=jax.ShapeDtypeStruct((rows, ow.shape[-1]), bf16),
        in_specs=[any_spec] * 5 + [vmem, pl.BlockSpec(memory_space=pltpu.SMEM), vmem],
        out_specs=vmem,
        scratch_shapes=[
            pltpu.VMEM((rows, depth), bf16),
            pltpu.VMEM((NU, 2, NY, NZ, 2, 64, 128), bf16),
            pltpu.VMEM((NY, NZ, 2, 16, 128), bf16),
            pltpu.VMEM((128, depth), bf16),
            pltpu.VMEM(ow.shape, bf16),
            pltpu.VMEM((NU, rows, 256), bf16),
            pltpu.VMEM((NH, rows, 128), f32),
            pltpu.VMEM((NH, 8, rows), f32),
            pltpu.VMEM((NH, 8, 128), f32),
            pltpu.VMEM((NH, 128, 128), f32),
            pltpu.VMEM((2, 2, 2, 72, 128), f32),
            pltpu.VMEM((2, NZ, 2, 80, 128), bf16),
            pltpu.VMEM((2, NY, 2, 80, 128), bf16),
            pltpu.VMEM((2, 2, 64, 128), bf16),
            pltpu.VMEM((NH, 128, 128), bf16),
            pltpu.VMEM((NH, rows, 128), f32),
            pltpu.VMEM((NH, rows, 128), bf16),
            pltpu.VMEM((NH, NX, rows, 128), bf16),
            pltpu.VMEM((rows, ow.shape[-1]), f32),
            dma((2 * NU + 3,)), dma((NB, 67)), dma((NB, 4)), dma((12,)), dma((2,)),
            dma((NB + 1,)), dma((NB + 1,)),
            dma((2, 2)), dma((2,)), dma((2, 8)), dma((2,)), dma((2, 4)), dma((2, 2)),
            dma((NH,)), dma((NH, 4)),
        ],
        compiler_params=pltpu.CompilerParams(
            collective_id=0, has_side_effects=True, vmem_limit_bytes=63 * 1024 * 1024
        ),
    )(tokens, wq, wk, wv, ow, gate, rate, gain)


def on_device(tokens, wq, wk, wv, wg, decay_rate, norm_gain, out_weight):
    ow = out_weight.reshape(NX, NH, 128, out_weight.shape[1])
    return fused(tokens, wq, wk, wv, ow, wg.T, decay_rate, norm_gain.reshape(NH, 128))


def solution(mesh):
    return jax.shard_map(
        on_device,
        mesh=mesh,
        in_specs=(
            P("seq", None), P("seq", "tp"), P("seq", "tp"), P("seq", "tp"), P("seq", "tp"),
            P("tp"), P("tp"), P(None, "tp"),
        ),
        out_specs=P("seq", "tp"),
        check_vma=False,
    )
```

```python
import jax
import jax.numpy as jnp
from jax import lax
from jax.experimental import pallas as pl
from jax.experimental.pallas import tpu as pltpu
from jax.sharding import PartitionSpec as P

NX, NY, NZ = 4, 4, 8
MESH = pl.DeviceIdType.MESH
UNITS = (
    ((1, 0), (2, 0)),
    ((1, 1), (2, 1)),
    ((1, 2), (2, 2)),
    ((1, 3), (2, 3)),
    ((0, 0), (0, 1)),
    ((0, 2), (0, 3)),
)
NU = len(UNITS)
NH = 4
NB = NU // 2
A1, A2, B1, B2 = 0, 4, 12, 20


class Ring:
    def __init__(self, item, n, pos, nxt, prv, recv, send, split=True):
        self.item, self.n, self.pos = item, n, pos
        self.nxt, self.prv, self.recv_sem, self.send_sem = nxt, prv, recv, send
        self.split = split

    def legs(self, r):
        last = r == self.n // 2 - 1
        parts = ((None, None), (0, 1))[last and self.split]
        dirs = (0,) if last and not self.split else (0, 1)
        return [(d, parts[d]) for d in dirs]

    def copy(self, idx, part, r, d):
        ref = self.item(lax.rem(idx + 2 * self.n, self.n), part)
        return pltpu.make_async_remote_copy(
            src_ref=ref,
            dst_ref=ref,
            send_sem=self.send_sem,
            recv_sem=self.recv_sem(2 * r + d),
            device_id=(self.nxt, self.prv)[d],
            device_id_type=MESH,
        )

    def send(self, r):
        for d, part in self.legs(r):
            self.copy(self.pos - r if d == 0 else self.pos + r, part, r, d).start()

    def recv(self, r):
        for d, part in self.legs(r):
            self.copy(
                self.pos - 1 - r if d == 0 else self.pos + 1 + r, part, r, d
            ).wait_recv()


class Direct:
    n = 2

    def __init__(self, item, pos, peers, recv, send):
        self.item, self.pos, self.peers = item, pos, peers
        self.recv_sem, self.send_sem = recv, send

    def copy(self, idx, d):
        ref = self.item(idx, None)
        return pltpu.make_async_remote_copy(
            src_ref=ref,
            dst_ref=ref,
            send_sem=self.send_sem,
            recv_sem=self.recv_sem(d - 1),
            device_id=self.peers[d - 1],
            device_id_type=MESH,
        )

    def send(self, r):
        for d in range(1, len(self.peers) + 1):
            self.copy(self.pos, d).start()

    def recv(self, r):
        for d in range(1, len(self.peers) + 1):
            self.copy(self.pos - d, d).wait_recv()


def thirds(v):
    hi = v.astype(jnp.bfloat16).astype(jnp.float32)
    mid = (v - hi).astype(jnp.bfloat16).astype(jnp.float32)
    return hi, mid, v - hi - mid


def kernel(
    tok_hbm, wq_hbm, wk_hbm, wv_hbm, ow_hbm, gate_ref, rate_ref, gain_ref,
    out_ref,
    tok, w, gb, gt, ow, proj, wcol, wrow, total, loc, swap, tz, ty, hand, state, local,
    qs, nb, acc,
    load_sem, recv_sem, send_sem, grecv_sem, gsend_sem, pair_send, pair_recv,
    swap_sem, zs_sem, zr_sem, ys_sem, yr_sem, hand_sem, xs_sem, xr_sem,
):
    x = lax.axis_index("tp")
    s = lax.axis_index("seq")
    y, z, c = s // (2 * NZ), lax.rem(s // 2, NZ), lax.rem(s, 2)

    def seq_id(yy, zz, cc):
        return {"seq": (lax.rem(yy + NY, NY) * NZ + lax.rem(zz + NZ, NZ)) * 2 + cc}

    yp, ym = seq_id(y + 1, z, c), seq_id(y - 1, z, c)
    zp, zm = seq_id(y, z + 1, c), seq_id(y, z - 1, c)
    mate = seq_id(y, z, 1 - c)
    y_peers = [seq_id(y + d, z, c) for d in range(1, NY)]
    z_peers = [seq_id(y, z + d, c) for d in range(1, NZ)]
    xp, xm = {"tp": lax.rem(x + 1, NX)}, {"tp": lax.rem(x + NX - 1, NX)}

    loads = []
    for u, tiles in enumerate(UNITS):
        for t, (m, h) in enumerate(tiles):
            src = (wq_hbm, wk_hbm, wv_hbm)[m].at[:, h * 128 : (h + 1) * 128]
            loads.append(
                pltpu.make_async_copy(src, w.at[u, t, y, z, c], load_sem.at[u * 2 + t])
            )
    for cp in loads:
        cp.start()
    tok_load = pltpu.make_async_copy(tok_hbm, tok, load_sem.at[2 * NU + 1])
    ow_load = pltpu.make_async_copy(ow_hbm, ow, load_sem.at[2 * NU + 2])

    barrier = pltpu.get_barrier_semaphore()
    partners = z_peers + y_peers + [mate, xp, xm]
    for dev in partners:
        pl.semaphore_signal(barrier, inc=1, device_id=dev, device_id_type=MESH)
    pl.semaphore_wait(barrier, len(partners))
    tok_load.start()
    ow_load.start()

    def rows(part):
        return slice(None) if part is None else pl.ds(part * 32, 32)

    def piece(b, tile, yy, zz, part):
        return w.at[pl.ds(2 * b, 2), tile, lax.rem(yy + NY, NY), lax.rem(zz + NZ, NZ), c, rows(part)]

    def rings(b):
        made = []
        base = 0

        def make(item, along_y, wait, k):
            nonlocal base
            first = base
            recv, send = lambda i: recv_sem.at[b, first + i], send_sem.at[b, k]
            if along_y:
                ring = Direct(item, y, y_peers, recv, send)
                base += NY - 1
            else:
                ring = Ring(item, NZ, z, zp, zm, recv, send)
                base += NZ
            made.append((wait, ring))

        make(lambda i, p: piece(b, 0, i, z, p), True, 0, 0)
        make(lambda i, p: piece(b, 1, y, i, p), False, 0, 1)
        for d in (0, 1, -1, 2):
            make(lambda i, p, d=d: piece(b, 0, y + d, i, p), False, min(abs(d), 1), 2)
        for d in (0, 1, -1, 2, -2, 3, -3, 4):
            make(lambda i, p, d=d: piece(b, 1, i, z + d, p), True, abs(d), 3)
        return made

    g1 = Direct(lambda i, p: gb.at[lax.rem(i + NY, NY), z, c], y, y_peers,
                lambda i: grecv_sem.at[i], gsend_sem.at[0])
    g2 = Direct(lambda i, p: gb.at[:, lax.rem(i + NZ, NZ), c], z, z_peers,
                lambda i: grecv_sem.at[4 + i], gsend_sem.at[1])

    def to_mate(ref, k):
        pltpu.make_async_remote_copy(
            src_ref=ref, dst_ref=ref, send_sem=pair_send.at[k], recv_sem=pair_recv.at[k],
            device_id=mate, device_id_type=MESH,
        ).start()

    def hop(ring, r):
        if r > 0:
            ring.recv(r - 1)
        if r < ring.n // 2:
            ring.send(r)

    def load_gate():
        k = lax.broadcasted_iota(jnp.int32, (64, 128), 0)
        lane = lax.broadcasted_iota(jnp.int32, (64, 128), 1)
        pick = jnp.where(lane == k + 64 * c, 1.0, 0.0).astype(jnp.bfloat16)
        turned = lax.dot_general(
            gate_ref[...], pick, (((1,), (0,)), ((), ())), preferred_element_type=jnp.float32
        )
        gb[y, z, c] = jnp.concatenate(
            [turned, jnp.zeros((12, 128), jnp.float32)], axis=0
        ).astype(jnp.bfloat16)

    def column(b, zz):
        to_mate(w.at[pl.ds(2 * b, 2), :, :, lax.rem(zz + NZ, NZ), c], b)

    def gate_round(k):
        if k == 0:
            g1.send(0)
        elif k == 1:
            g1.recv(0)
            g2.send(0)
            to_mate(g2.item(z, None), NB)
        else:
            g2.recv(0)
            for d in range(1, NZ):
                to_mate(g2.item(z - d, None), NB)

    def weight_round(k, b):
        if k == 0:
            for i in range(2):
                for t in range(2):
                    own = w.at[2 * b + i, t, y, z, c]
                    pltpu.make_async_copy(own, own, load_sem.at[b * 4 + 2 * i + t]).wait()

        todo = [(ring, k - wait) for wait, ring in rings(b)]
        for ring, r in todo:
            if 0 < r <= ring.n // 2:
                ring.recv(r - 1)
            if 0 <= r < ring.n // 2:
                ring.send(r)
        if k >= 1:
            d = k - 1
            for at in {0: (z,), 4: (z + 4,)}.get(d, (z + d, z - d)):
                column(b, at)

    def pair_done(ref, k):
        return pltpu.make_async_remote_copy(
            src_ref=ref, dst_ref=ref, send_sem=pair_send.at[k], recv_sem=pair_recv.at[k],
            device_id=mate, device_id_type=MESH,
        )

    def sent(ref, sem):
        pltpu.make_async_remote_copy(
            src_ref=ref, dst_ref=ref, send_sem=sem, recv_sem=pair_recv.at[0],
            device_id=mate, device_id_type=MESH,
        ).wait_send()

    def finish():
        pair_done(gb.at[:, :, c], NB).wait_send()
        sent(gb.at[pl.ds(0, 3), z, c], gsend_sem.at[0])
        sent(gb.at[:, pl.ds(0, 7), c], gsend_sem.at[1])

        def one(b, _):
            two = pl.ds(2 * b, 2)
            pair_done(w.at[two, :, :, :, c], b).wait_send()
            sent(w.at[two, 0, pl.ds(0, 3), z, c], send_sem.at[b, 0])
            sent(w.at[two, 1, y, pl.ds(0, 7), c], send_sem.at[b, 1])
            sent(w.at[two, 0, :, pl.ds(0, 7), c], send_sem.at[b, 2])
            sent(w.at[two, 1, pl.ds(0, 3), :, c], send_sem.at[b, 3])
            return 0

        lax.fori_loop(0, NB, one, 0)

    def project(u):
        rhs = jnp.concatenate(
            [w[u, 0].reshape(4096, 128), w[u, 1].reshape(4096, 128)], axis=1
        )

        def chunk(r, _):
            at = pl.ds(pl.multiple_of(r * 256, 256), 256)
            proj[u, at, :] = jnp.dot(
                tok[at, :], rhs, preferred_element_type=jnp.float32
            ).astype(jnp.bfloat16)
            return 0

        lax.fori_loop(0, 3, chunk, 0)

    def gate():
        gt[...] = jnp.zeros_like(gt)
        for yy in range(NY):
            for zz in range(NZ):
                k = (yy * NZ + zz) * 128
                gt[0:16, k : k + 128] = gb[yy, zz, 0] + gb[yy, zz, 1]
        logit = lax.dot_general(
            tok[...], gt[...], (((1,), (1,)), ((), ())), preferred_element_type=jnp.float32
        )
        logit = logit.T[0:8, :]
        soft = jnp.maximum(logit, 0.0) + jnp.log1p(jnp.exp(-jnp.abs(logit)))
        head = lax.broadcasted_iota(jnp.int32, (8, 128), 0)
        rate = jnp.zeros((8, 128), jnp.float32)
        for h in range(NH):
            rate = jnp.where(head == h, rate_ref[h], rate)
        decay = -rate[:, 0:1] * soft
        hi, mid, lo = thirds(decay)
        parts = jnp.concatenate([hi, mid, lo, jnp.zeros_like(lo)], axis=0).astype(jnp.bfloat16)
        before = lax.broadcasted_iota(jnp.int32, (768, 768), 0)
        after = lax.broadcasted_iota(jnp.int32, (768, 768), 1)
        upper = jnp.where(before <= after, 1.0, 0.0).astype(jnp.bfloat16)
        sums = jnp.dot(parts, upper, preferred_element_type=jnp.float32)
        within = sums[0:8] + sums[8:16] + sums[16:24]
        column = jnp.concatenate([within, jnp.zeros((120, 768), jnp.float32)], axis=0).T
        for h in range(NH):
            wrow[h] = jnp.broadcast_to(within[h : h + 1, :], (8, 768))
            wcol[h] = jnp.broadcast_to(column[:, h : h + 1], (768, 128))
            total[h] = jnp.broadcast_to(within[h : h + 1, 767:768], (8, 128))

    def half(k):
        return pl.ds(pl.multiple_of(k * 64, 64), 64)

    def local_state(u, h):
        key = proj[u, :, 0:128].astype(jnp.float32)
        scaled = (jnp.exp(total[h, 0:1, :] - wcol[h]) * key).astype(jnp.bfloat16)
        loc[h] = lax.dot_general(
            scaled, proj[u, :, 128:256], (((0,), (0,)), ((), ())),
            preferred_element_type=jnp.float32,
        )
        q, i = h // 2, lax.rem(h, 2)
        swap[q, 0, i, 0:64, :] = loc[h, half(1 - c), :]
        swap[q, 0, i, 64:72, :] = total[h]

    def swap_copy(q):
        return pltpu.make_async_remote_copy(
            src_ref=swap.at[q, 0], dst_ref=swap.at[q, 1], send_sem=swap_sem.at[q, 0],
            recv_sem=swap_sem.at[q, 1], device_id=mate, device_id_type=MESH,
        )

    def hand_copy(q, k):
        return pltpu.make_async_remote_copy(
            src_ref=hand.at[q], dst_ref=state.at[pl.ds(2 * q, 2), half(k)],
            send_sem=hand_sem.at[q, 0], recv_sem=hand_sem.at[q, 1],
            device_id=mate, device_id_type=MESH,
        )

    def all_z(q, d, src):
        ref = tz.at[q, lax.rem(src + NZ, NZ)]
        return pltpu.make_async_remote_copy(
            src_ref=ref, dst_ref=ref, send_sem=zs_sem.at[q], recv_sem=zr_sem.at[q, d - 1],
            device_id=seq_id(y, z + d, c), device_id_type=MESH,
        )

    def all_y(q, d, src):
        ref = ty.at[q, lax.rem(src + NY, NY)]
        return pltpu.make_async_remote_copy(
            src_ref=ref, dst_ref=ref, send_sem=ys_sem.at[q], recv_sem=yr_sem.at[q, d - 1],
            device_id=seq_id(y + d, z, c), device_id_type=MESH,
        )

    def x_ring(h):
        def item(i, p):
            return nb.at[h, i] if p is None else nb.at[h, i, pl.ds(p * 384, 384)]

        return Ring(item, NX, x, xp, xm, lambda i: xr_sem.at[h, i], xs_sem.at[h])

    def pack(ref, at, i, value, log):
        hi, mid, lo = thirds(log)
        row = lax.broadcasted_iota(jnp.int32, (16, 128), 0)
        tail = jnp.where(row == 0, hi, jnp.where(row == 1, mid, jnp.where(row == 2, lo, 0.0)))
        ref[at, i, 0:64, :] = value.astype(jnp.bfloat16)
        ref[at, i, 64:80, :] = tail.astype(jnp.bfloat16)

    def unpack(ref, at, i):
        tail = ref[at, i, 64:80, :].astype(jnp.float32)
        return ref[at, i, 0:64, :].astype(jnp.float32), jnp.sum(tail, axis=0, keepdims=True)

    def pair(q, i):
        h = 2 * q + i
        mine, theirs = loc[h, half(c), :], swap[q, 1, i, 0:64, :]
        own, other = total[h, 0:1, :], swap[q, 1, i, 64:65, :]
        first = c == 0
        return (
            jnp.where(first, mine, theirs), jnp.where(first, own, other),
            jnp.where(first, theirs, mine), jnp.where(first, other, own),
        )

    def below(ref, i, n, limit):
        acc_s = jnp.zeros((64, 128), jnp.float32)
        acc_a = jnp.zeros((1, 128), jnp.float32)
        kept = (acc_s, acc_a)
        for at in range(n):
            s_at, a_at = unpack(ref, at, i)
            acc_s, acc_a = jnp.exp(a_at) * acc_s + s_at, acc_a + a_at
            kept = tuple(
                jnp.where(at < limit, new, old) for new, old in zip((acc_s, acc_a), kept)
            )
        return kept, (acc_s, acc_a)

    def scan_step(k, q):
        if k == 1:
            swap_copy(q).wait_recv()
            for i in range(2):
                s0, a0, s1, a1 = pair(q, i)
                pack(tz.at[q], z, i, jnp.exp(a1) * s0 + s1, a0 + a1)
            for d in (4, 3, 5, 2, 6, 1, 7):
                all_z(q, d, z).start()
        elif k == 2:
            for d in range(1, NZ):
                all_z(q, d, z - d).wait_recv()
            for i in range(2):
                _, (row_s, row_a) = below(tz.at[q], i, NZ, z)
                pack(ty.at[q], y, i, row_s, row_a)
            for d in (2, 1, 3):
                all_y(q, d, y).start()
        elif k == 3:
            for d in range(1, NY):
                all_y(q, d, y - d).wait_recv()
            first = c == 0
            for i in range(2):
                (in_s, in_a), _ = below(tz.at[q], i, NZ, z)
                (row_s, _), _ = below(ty.at[q], i, NY, y)
                p0 = jnp.exp(in_a) * row_s + in_s
                s0, a0, _, _ = pair(q, i)
                p1 = jnp.exp(a0) * p0 + s0
                hand[q, i] = jnp.where(first, p1, p0).astype(jnp.bfloat16)
                state[2 * q + i, half(c), :] = jnp.where(first, p0, p1).astype(jnp.bfloat16)
            hand_copy(q, c).start()
        else:
            hand_copy(q, 1 - c).wait_recv()

    def attention(u, i, h):
        kv = h
        for r in range(3):
            lo, n = r * 256, (r + 1) * 256
            query = proj[u, lo:n, i * 128 : (i + 1) * 128]
            scores = lax.dot_general(
                query, proj[kv, 0:n, 0:128], (((1,), (1,)), ((), ())),
                preferred_element_type=jnp.float32,
            )
            col = wcol[h, lo:n, :]
            gap = jnp.concatenate([col] * (n // 128), axis=1) - wrow[h, 0:1, 0:n]
            t_at = lax.broadcasted_iota(jnp.int32, (256, n), 0) + lo
            s_at = lax.broadcasted_iota(jnp.int32, (256, n), 1)
            causal = s_at <= t_at
            attn = jnp.where(
                causal, scores * jnp.exp(jnp.where(causal, gap, 0.0)), 0.0
            ).astype(jnp.bfloat16)
            local[h, lo:n, :] = jnp.dot(
                attn, proj[kv, 0:n, 128:256], preferred_element_type=jnp.float32
            )
            qs[h, lo:n, :] = (jnp.exp(col) * query.astype(jnp.float32)).astype(jnp.bfloat16)

    def normed(h):
        out = local[h] + jnp.dot(qs[h], state[h], preferred_element_type=jnp.float32)
        scale = lax.rsqrt(jnp.mean(out * out, axis=-1, keepdims=True) + 1e-05)
        nb[h, x] = (out * scale * gain_ref[pl.ds(h, 1), :]).astype(jnp.bfloat16)
        x_ring(h).send(0)

    def mix(h, first, last):
        weight = ow[:, h].reshape(512, 1024)

        def chunk(r, _):
            at = pl.ds(pl.multiple_of(r * 256, 256), 256)
            lhs = jnp.concatenate([nb[h, i, at, :] for i in range(NX)], axis=1)
            part = jnp.dot(lhs, weight, preferred_element_type=jnp.float32)
            if not first:
                part = part + acc[at, :]
            if last:
                out_ref[at, :] = part.astype(jnp.bfloat16)
            else:
                acc[at, :] = part
            return 0

        lax.fori_loop(0, 3, chunk, 0)

    def arrived(b):
        pair_done(w.at[pl.ds(2 * b, 2), :, :, :, 1 - c], b).wait_recv()

    def key_value(u):
        project(u)
        local_state(u, u)

    def slot(t, _):
        for k in range(5, -1, -1):
            @pl.when((t >= k) & (t < k + NB))
            def _():
                weight_round(k, t - k)

        for k in range(3):
            pl.when(t == k)(lambda k=k: gate_round(k))

        @pl.when(t == 3)
        def _():
            pair_done(gb.at[:, :, 1 - c], NB).wait_recv()
            tok_load.wait()
            gate()

        @pl.when(t == 6)
        def _():
            scan_step(1, 0)

        @pl.when(t >= 5)
        def _():
            b = t - 5
            arrived(b)
            key_value(2 * b)
            key_value(2 * b + 1)
            swap_copy(b).start()

        return 0

    def gathered(h):
        hop(x_ring(h), 2)
        mix(h, h == 0, h == NH - 1)

    load_gate()
    lax.fori_loop(0, 7, slot, 0)
    weight_round(5, NB - 1)
    scan_step(2, 0)
    scan_step(1, 1)
    arrived(2)
    project(4)
    attention(4, 0, 0)
    scan_step(3, 0)
    attention(4, 1, 1)
    scan_step(4, 0)
    normed(0)
    normed(1)
    scan_step(2, 1)
    project(5)
    attention(5, 0, 2)
    scan_step(3, 1)
    hop(x_ring(0), 1)
    scan_step(4, 1)
    normed(2)
    hop(x_ring(1), 1)
    attention(5, 1, 3)
    normed(3)
    ow_load.wait()
    gathered(0)
    hop(x_ring(2), 1)
    gathered(1)
    hop(x_ring(3), 1)
    gathered(2)
    gathered(3)
    finish()

    def end(h, _):
        sent(nb.at[h, pl.ds(0, 3)], xs_sem.at[h])
        return 0

    lax.fori_loop(0, NH, end, 0)
    for q in range(2):
        swap_copy(q).wait_send()
        sent(tz.at[q, pl.ds(0, 7)], zs_sem.at[q])
        sent(ty.at[q, pl.ds(0, 3)], ys_sem.at[q])
        hand_copy(q, c).wait_send()


def fused(tokens, wq, wk, wv, ow, gate, rate, gain):
    rows, depth = tokens.shape
    any_spec = pl.BlockSpec(memory_space=pl.ANY)
    vmem = pl.BlockSpec(memory_space=pltpu.VMEM)
    bf16, f32, dma = jnp.bfloat16, jnp.float32, pltpu.SemaphoreType.DMA
    return pl.pallas_call(
        kernel,
        out_shape=jax.ShapeDtypeStruct((rows, ow.shape[-1]), bf16),
        in_specs=[any_spec] * 5 + [vmem, pl.BlockSpec(memory_space=pltpu.SMEM), vmem],
        out_specs=vmem,
        scratch_shapes=[
            pltpu.VMEM((rows, depth), bf16),
            pltpu.VMEM((NU, 2, NY, NZ, 2, 64, 128), bf16),
            pltpu.VMEM((NY, NZ, 2, 16, 128), bf16),
            pltpu.VMEM((128, depth), bf16),
            pltpu.VMEM(ow.shape, bf16),
            pltpu.VMEM((NU, rows, 256), bf16),
            pltpu.VMEM((NH, rows, 128), f32),
            pltpu.VMEM((NH, 8, rows), f32),
            pltpu.VMEM((NH, 8, 128), f32),
            pltpu.VMEM((NH, 128, 128), f32),
            pltpu.VMEM((2, 2, 2, 72, 128), f32),
            pltpu.VMEM((2, NZ, 2, 80, 128), bf16),
            pltpu.VMEM((2, NY, 2, 80, 128), bf16),
            pltpu.VMEM((2, 2, 64, 128), bf16),
            pltpu.VMEM((NH, 128, 128), bf16),
            pltpu.VMEM((NH, rows, 128), f32),
            pltpu.VMEM((NH, rows, 128), bf16),
            pltpu.VMEM((NH, NX, rows, 128), bf16),
            pltpu.VMEM((rows, ow.shape[-1]), f32),
            dma((2 * NU + 3,)), dma((NB, 67)), dma((NB, 4)), dma((12,)), dma((2,)),
            dma((NB + 1,)), dma((NB + 1,)),
            dma((2, 2)), dma((2,)), dma((2, 8)), dma((2,)), dma((2, 4)), dma((2, 2)),
            dma((NH,)), dma((NH, 4)),
        ],
        compiler_params=pltpu.CompilerParams(
            collective_id=0, has_side_effects=True, vmem_limit_bytes=63 * 1024 * 1024
        ),
    )(tokens, wq, wk, wv, ow, gate, rate, gain)


def on_device(tokens, wq, wk, wv, wg, decay_rate, norm_gain, out_weight):
    ow = out_weight.reshape(NX, NH, 128, out_weight.shape[1])
    return fused(tokens, wq, wk, wv, ow, wg.T, decay_rate, norm_gain.reshape(NH, 128))


def solution(mesh):
    return jax.shard_map(
        on_device,
        mesh=mesh,
        in_specs=(
            P("seq", None), P("seq", "tp"), P("seq", "tp"), P("seq", "tp"), P("seq", "tp"),
            P("tp"), P("tp"), P(None, "tp"),
        ),
        out_specs=P("seq", "tp"),
        check_vma=False,
    )
```
